256 devices in a mesh: rep: 1, dp: 256 (over x, y, z, core).
Axes of the slice: x: 4, y: 4, z: 8, core: 2. Of those that a mesh axis runs over, the one named last changes fastest.
Arguments:
- x: bfloat16 [256, 1024, 768], P(('rep', 'dp'))
- dy: bfloat16 [256, 1024, 768], P(('rep', 'dp'))
- w_gate: bfloat16 [2, 768, 6144], P(None, 'dp')
- w_up: bfloat16 [2, 768, 6144], P(None, 'dp')
- w_down: bfloat16 [2, 6144, 768], P(None, 'dp')
- m_w_gate: float32 [2, 768, 6144], P(None, 'dp')
- m_w_up: float32 [2, 768, 6144], P(None, 'dp')
- m_w_down: float32 [2, 6144, 768], P(None, 'dp')
- v_w_gate: float32 [2, 768, 6144], P(None, 'dp')
- v_w_up: float32 [2, 768, 6144], P(None, 'dp')
- v_w_down: float32 [2, 6144, 768], P(None, 'dp')
Outputs:
- output 1: bfloat16 [2, 768, 6144], P('rep', 'dp')
- output 2: bfloat16 [2, 768, 6144], P('rep', 'dp')
- output 3: bfloat16 [2, 6144, 768], P('rep', 'dp')
- output 4: float32 [2, 768, 6144], P('rep', 'dp')
- output 5: float32 [2, 768, 6144], P('rep', 'dp')
- output 6: float32 [2, 6144, 768], P('rep', 'dp')
- output 7: float32 [2, 768, 6144], P('rep', 'dp')
- output 8: float32 [2, 768, 6144], P('rep', 'dp')
- output 9: float32 [2, 6144, 768], P('rep', 'dp')
All inputs are finite; a program needn't handle non-finite values.
Results may differ from the reference program's by a relative error of at most 0.022.
Values are sent between devices in bfloat16 or wider.
A program may use at most 768 MiB of HBM per device.

```python
import jax
import jax.numpy as jnp
from jax import lax

SEQUENCES = 256
TOKENS = 1024
D = 768
FF = 6144
LAYERS = 2
NAMES = ("w_gate", "w_up", "w_down")
SHAPES = {"w_gate": (LAYERS, D, FF), "w_up": (LAYERS, D, FF), "w_down": (LAYERS, FF, D)}


def bump(key, n, height):
    away = (jnp.arange(n, dtype=jnp.int32) - jax.random.randint(key, (), 0, n, jnp.int32)) % n
    return jnp.where(away < n // 8, height, 1.0)


def together(key, own, strength):
    shared = jax.random.normal(key, own.shape[1:], jnp.float32)
    return (own + strength * shared) * lax.rsqrt(1 + strength * strength)


def setup_inputs(seed: int = 0, part: int = 0) -> dict:
    kx, kdy, ka, kb, kz, kf, kh, kl, *keys = jax.random.split(jax.random.key(seed), 8 + 3 * len(NAMES))
    kx, kdy, ka, kb = (jax.random.fold_in(k, part) for k in (kx, kdy, ka, kb))
    kw, km, kv = (keys[i::3] for i in range(3))
    shape = (SEQUENCES, TOKENS, D)
    much_x, much_dy = jax.random.uniform(kz, (2,), jnp.float32, 0.0, 1.0)
    loud = 2.0 ** jax.random.uniform(jax.random.fold_in(kz, 1), (), jnp.float32, -1.0, 2.0)
    layers = 2.0 ** jax.random.uniform(kl, (LAYERS, 1, 1), jnp.float32, -1.0, 1.0)
    x = together(ka, jax.random.normal(kx, shape, jnp.float32), much_x) * bump(kf, D, 4.0)
    dy = together(kb, jax.random.normal(kdy, shape, jnp.float32), much_dy)
    drawn = {"x": x.astype(jnp.bfloat16), "dy": (loud * dy * (SEQUENCES * TOKENS) ** -0.5).astype(jnp.bfloat16)}
    for key, name in zip(kw, NAMES, strict=True):
        w = jax.random.normal(key, SHAPES[name], jnp.float32) * SHAPES[name][1] ** -0.5
        drawn[name] = (w * {"w_gate": 1.0, "w_up": bump(kh, FF, 4.0), "w_down": layers}[name]).astype(jnp.bfloat16)
    for key, name in zip(km, NAMES, strict=True):
        drawn[f"m_{name}"] = 0.1 * jax.random.normal(key, SHAPES[name], jnp.float32)
    for key, name in zip(kv, NAMES, strict=True):
        drawn[f"v_{name}"] = jax.random.uniform(key, SHAPES[name], jnp.float32, 0.005, 0.015)
    return drawn


def matmul(a, w):
    return jnp.dot(a, w, preferred_element_type=jnp.float32).astype(jnp.bfloat16)


def normed(h):
    wide = h.astype(jnp.float32)
    scale = lax.rsqrt(jnp.mean(wide**2, -1, keepdims=True) + 1e-6)
    return (wide * scale).astype(jnp.bfloat16)


def layer(h, w):
    a = normed(h)
    gate = jnp.dot(a, w["w_gate"], preferred_element_type=jnp.float32)
    up = jnp.dot(a, w["w_up"], preferred_element_type=jnp.float32)
    return h + matmul((jax.nn.silu(gate) * up).astype(jnp.bfloat16), w["w_down"])


def adamw(w, m, v, g):
    m = 0.9 * m + 0.1 * g
    v = 0.95 * v + 0.05 * g * g
    step = m * lax.rsqrt(v + 1e-8) + 0.1 * w
    return (w - 0.02 * step).astype(jnp.bfloat16), m, v


def clipped(gradients, sum_of_squares, count):
    factor = jnp.minimum(1.0, 0.5 * lax.rsqrt(sum_of_squares / count + 1e-30))
    return [g * factor for g in gradients]


def stack(weights, h):
    return lax.scan(lambda h, w: (layer(h, w), None), h, weights)[0]


def reference(x, dy, w_gate, w_up, w_down, m_w_gate, m_w_up, m_w_down, v_w_gate, v_w_up, v_w_down):
    weights = dict(zip(NAMES, (w_gate, w_up, w_down), strict=True))

    def take(so_far, sequence):
        h, by_y = sequence
        _, back = jax.vjp(lambda w: stack(w, h), weights)
        return jax.tree.map(lambda total, term: total + term.astype(jnp.float32), so_far, back(by_y)[0]), None

    none_yet = {name: jnp.zeros(w.shape, jnp.float32) for name, w in weights.items()}
    by_weights, _ = lax.scan(take, none_yet, (x, dy))
    gradients = [by_weights[name].astype(jnp.bfloat16).astype(jnp.float32) for name in NAMES]
    gradients = clipped(gradients, sum(jnp.sum(g * g) for g in gradients), sum(g.size for g in gradients))
    new = [
        adamw(w.astype(jnp.float32), m, v, g)
        for w, m, v, g in zip((w_gate, w_up, w_down), (m_w_gate, m_w_up, m_w_down), (v_w_gate, v_w_up, v_w_down), gradients, strict=True)
    ]
    return tuple(one[which] for which in range(3) for one in new)
```

```python
import functools
import itertools
import jax
import jax.numpy as jnp
from jax import lax
from jax.experimental import pallas as pl
from jax.experimental.pallas import tpu as pltpu
from jax.sharding import PartitionSpec as P

DIMS = (4, 4, 8, 2)
T = 3
CH, CL = 24, 256
ORDERS = ((0, 1, 2), (1, 2, 0), (2, 0, 1))
f32, bf16 = jnp.float32, jnp.bfloat16
ALL = slice(None)
LANES = CL // 2


def coords():
    me = lax.axis_index("dp")
    c = lax.rem(me, DIMS[3])
    r = lax.div(me, DIMS[3])
    z = lax.rem(r, DIMS[2])
    r = lax.div(r, DIMS[2])
    y = lax.rem(r, DIMS[1])
    x = lax.div(r, DIMS[1])
    return [x, y, z, c]


def flat(co):
    return ((co[0] * DIMS[1] + co[1]) * DIMS[2] + co[2]) * DIMS[3] + co[3]


def moved(co, axis, by):
    n = DIMS[axis]
    out = list(co)
    out[axis] = lax.rem(co[axis] + (by + n), n)
    return out


def group_peers(co):
    zs = min(4, DIMS[2])
    base = lax.div(co[2], zs) * zs
    mine = lax.rem(co[2], zs) * DIMS[3] + co[3]
    return zs * DIMS[3], base, mine


def member(co, base, j):
    out = list(co)
    out[2] = base + lax.div(j, DIMS[3])
    out[3] = lax.rem(j, DIMS[3])
    return out


def greet(co, extra=()):
    barrier = pltpu.get_barrier_semaphore()
    peers = [moved(co, a, d) for a in range(3) for d in (1, -1)]
    peers += [co[:3] + [(co[3] + k) % DIMS[3]] for k in range(1, DIMS[3])]
    peers += list(extra)
    for peer in peers:
        pl.semaphore_signal(barrier, inc=1, device_id={"dp": flat(peer)})
    pl.semaphore_wait(barrier, len(peers))


def side(by):
    return (1 - by) // 2


def columns(half):
    return ALL if half is ALL else pl.ds(half * LANES, LANES)


def remote(src, dst, ssem, rsem, co):
    return pltpu.make_async_remote_copy(src_ref=src, dst_ref=dst, send_sem=ssem, recv_sem=rsem, device_id={"dp": flat(co)})


def at(ref, sel, core, cols=ALL):
    index = [ALL] + list(sel)
    if core is not ALL:
        index.append(core)
    if cols is not ALL:
        index += [ALL, cols]
    return ref.at[tuple(index)]


HOP = 3.0
RATE = 46.6e3
CHUNK_BYTES = T * CH * CL * 2


def gather_ticks(stream, ref, own, order, co, ssem, rsem, dsend, drecv, local, start=0.0):
    partner = co[:3] + [1 - co[3]]
    ticks, sends, d2d = [], [], []
    time = start
    n_copy = itertools.count()
    n_d2d = itertools.count()

    def forward(block):
        copy = remote(block, block, dsend.at[next(n_d2d)], drecv.at[0], partner)
        copy.start()
        d2d.append(copy)

    mine = at(ref, co[:3], co[3])
    keep = pltpu.make_async_copy(own, mine, local.at[0])
    arrived = []
    for k, axis in enumerate(order):
        n = DIMS[axis]
        done, last = order[:k], k == len(order) - 1
        blocks = 1
        for a in done:
            blocks *= DIMS[a]

        def block(pos, half=ALL, done=done, axis=axis):
            sel = [ALL if a in done else co[a] for a in range(3)]
            sel[axis] = pos
            cols = ALL
            if half is not ALL:
                if done:
                    h = DIMS[done[0]] // 2
                    sel[done[0]] = pl.ds(half * h, h)
                else:
                    cols = columns(half)
            return at(ref, sel, co[3], cols)

        for s in range(1, n // 2 + 1):
            final = s == n // 2

            def tick(k=k, s=s, axis=axis, final=final, last=last, block=block):
                came = list(arrived)
                arrived.clear()
                if k == 0 and s == 1:
                    keep.start()
                if k == 1 and s == 1:
                    keep.wait()
                for copy, got in came:
                    copy.wait_recv()
                for by in (1, -1):
                    pos = moved(co, axis, -by * (s - 1))[axis]
                    half = side(by) if final else ALL
                    target = block(pos, half)
                    source = target
                    if k == 0 and s == 1:
                        source = own.at[:, :, columns(half)]
                    i = next(n_copy)
                    copy = remote(source, target, ssem.at[i], rsem.at[i], moved(co, axis, by))
                    copy.start()
                    sends.append(copy)
                    got = block(moved(co, axis, -by * s)[axis], half)
                    arrived.append((copy, got))
                if last:
                    if s == 1:
                        forward(block(co[axis]))
                    else:
                        for copy, got in came:
                            forward(got)

            ticks.append((time, tick))
            time += HOP + blocks * CHUNK_BYTES * (0.5 if final else 1.0) / RATE

    def finish():
        for copy, got in arrived:
            copy.wait_recv()
            forward(got)

    def drain():
        half = at(ref, [ALL] * 3, 1 - co[3])
        pltpu.make_async_copy(half, half, drecv.at[0]).wait()
        for copy in sends + d2d:
            copy.wait_send()

    ticks.append((time, finish))
    ticks.append((time + 5.0, drain))
    return ticks


def run(ticks):
    for _, tick in sorted(ticks, key=lambda t: t[0]):
        tick()


def scatter_scratch(order):
    n2, n3 = DIMS[order[1]], DIMS[order[2]]
    whole = (T,) + DIMS[:3] + (CH, CL)
    return [
        pltpu.VMEM(whole, bf16),
        pltpu.VMEM(whole, bf16),
        pltpu.VMEM(whole, bf16),
        pltpu.VMEM((T, n2, n3, CH, CL), f32),
        pltpu.VMEM((T, n2, n3, CH, CL), bf16),
        pltpu.VMEM((T, n2, n3, CH, CL), bf16),
        pltpu.VMEM((T, n3, CH, CL), bf16),
        pltpu.SemaphoreType.DMA((3, DIMS[order[0]])),
        pltpu.SemaphoreType.DMA((2, 16)),
    ]


SCATTER_SCRATCH = 9


def scatter_ticks(partial, order, co, scratch, out, start=0.0):
    kept, other, came1, total, going, came2, came3, load, ring = scratch
    b1, b2, b3 = order
    n1, n2, n3 = (DIMS[a] for a in order)
    p1, p2, p3 = (co[a] for a in order)
    partner = co[:3] + [1 - co[3]]
    ticks, sends = [], []
    n_copy = itertools.count()
    time = start

    def sel(q, i=ALL, j=ALL):
        s = [ALL] * 3
        s[b1], s[b2], s[b3] = q, i, j
        return s

    def place(ref, s):
        return ref.at[tuple([ALL] + s)]

    offsets = [n1 // 2] + [d * k for k in range(n1 // 2 - 1, 0, -1) for d in (1, -1)] + [0]
    loads = {}

    def begin():
        for i, off in enumerate(offsets):
            q = moved(co, b1, off)[b1]
            here = pltpu.make_async_copy(at(partial, sel(q), co[3]), place(kept, sel(q)), load.at[0, i])
            there = remote(at(partial, sel(q), 1 - co[3]), place(other, sel(q)), load.at[1, i], load.at[2, i], partner)
            there.start()
            here.start()
            loads[off] = [here, there]
            sends.append(there)

    def ready(off):
        off = -off if off == -(n1 // 2) else off
        if off in loads:
            here, there = loads.pop(off)
            here.wait()
            there.wait_recv()

    def add(count, spots, dst, srcs):
        def body(m, _):
            spot = spots(m)
            for t in range(T):
                ref, index = dst(t, *spot)
                value = sum(r[i].astype(f32) for r, i in (s(t, *spot) for s in srcs))
                ref[index] = value.astype(ref.dtype)
            return 0

        lax.fori_loop(0, count, body, 0)

    def phase1(ref, q):
        def spot(t, i, j):
            s = sel(q, i, j)
            return ref, (t, s[0], s[1], s[2])

        return spot

    def phase2(ref, q):
        return lambda t, j: (ref, (t, q, j))

    def phase3(ref, q, first=()):
        return lambda t: (ref, (t,) + tuple(first) + (q,))

    def step(axis, n, p, s, sum_into, view, slots):
        out = []
        for by in (1, -1):
            off = by * (n // 2 + 1 - s)
            q = moved(co, axis, off)[axis]
            half = side(by) if s == 1 else ALL
            mine = side(by)
            sum_into(q, half, s, mine, off)
            if by == -1 and s == n // 2:
                slot = moved(co, axis, by + n // 2)[axis]
            else:
                slot = q
            i = next(n_copy)
            copy = remote(view(q, half), slots(slot, half), ring.at[0, i], ring.at[1, i], moved(co, axis, by))
            copy.start()
            sends.append(copy)
            out.append(copy)
        return out

    arrived = []

    def await_arrived():
        for copy in arrived:
            copy.wait_recv()
        arrived.clear()

    def halves(n, half):
        return (0, n) if half is ALL else (half * (n // 2), n // 2)

    def sum1(q, half, s, mine, off):
        ready(off)

        def part(lo, size, with_sum):
            def spots(m):
                return lo + lax.div(m, n3), lax.rem(m, n3)

            srcs = [phase1(kept, q), phase1(other, q)] + ([phase1(came1, q)] if with_sum else [])
            add(size * n3, spots, phase1(kept, q), srcs)

        if s == 1:
            part(*halves(n2, half), False)
        elif s == 2:
            part(*halves(n2, mine), True)
            part(*halves(n2, 1 - mine), False)
        else:
            part(0, n2, True)

    def cut1(ref):
        def view(q, half):
            lo, size = halves(n2, half)
            return place(ref, sel(q, ALL if half is ALL else pl.ds(lo, size)))

        return view

    def end1():
        await_arrived()
        ready(0)
        mine, far = p1, moved(co, b1, n1 // 2)[b1]
        add(n2 * n3, lambda m: (lax.div(m, n3), lax.rem(m, n3)), lambda t, i, j: (total, (t, i, j)),
            [phase1(kept, mine), phase1(other, mine), phase1(came1, mine), phase1(came1, far)])

    def sum2(q, half, s, mine, off):
        def part(lo, size, with_sum):
            srcs = [phase2(total, q)] + ([phase2(came2, q)] if with_sum else [])
            add(size, lambda m: (lo + m,), phase2(going, q), srcs)

        if s == 1:
            part(*halves(n3, half), False)
        elif s == 2:
            part(*halves(n3, mine), True)
            part(*halves(n3, 1 - mine), False)
        else:
            part(0, n3, True)

    def cut2(ref):
        def view(q, half):
            lo, size = halves(n3, half)
            return ref.at[:, q, pl.ds(lo, size)]

        return view

    def end2():
        await_arrived()
        far = moved(co, b2, n2 // 2)[b2]
        add(n3, lambda m: (m,), phase2(total, p2), [phase2(total, p2), phase2(came2, p2), phase2(came2, far)])

    def sum3(q, half, s, mine, off):
        def part(cols, with_sum):
            for t in range(T):
                value = total[t, p2, q, :, cols]
                if with_sum:
                    value = value + came3[t, q, :, cols].astype(f32)
                going[t, p2, q, :, cols] = value.astype(bf16)

        if s == 1:
            part(columns(half), False)
        elif s == 2:
            part(columns(mine), True)
            part(columns(1 - mine), False)
        else:
            part(ALL, True)

    def end3():
        await_arrived()
        far = moved(co, b3, n3 // 2)[b3]
        for t in range(T):
            value = total[t, p2, p3] + came3[t, p3].astype(f32) + came3[t, far].astype(f32)
            out[t] = value.astype(bf16).astype(f32)

    def cut3(ref, first):
        def view(q, half):
            cols = columns(half)
            index = (ALL,) + tuple(first) + (q, ALL, cols)
            return ref.at[index]

        return view

    ticks.append((time, begin))
    time += 2.0
    phases = (
        (b1, n1, p1, sum1, cut1(kept), cut1(came1), end1, n2 * n3),
        (b2, n2, p2, sum2, cut2(going), cut2(came2), end2, n3),
        (b3, n3, p3, sum3, cut3(going, (p2,)), cut3(came3, ()), end3, 1),
    )
    for axis, n, p, sum_into, view, slots, end, blocks in phases:
        for s in range(1, n // 2 + 1):

            def tick(axis=axis, n=n, p=p, s=s, sum_into=sum_into, view=view, slots=slots):
                await_arrived()
                arrived.extend(step(axis, n, p, s, sum_into, view, slots))

            ticks.append((time, tick))
            time += HOP + 0.5 + blocks * CHUNK_BYTES * (0.5 if s == 1 else 1.0) / RATE
        ticks.append((time, end))
        time += 0.2

    def drain():
        for copy in sends:
            copy.wait_send()

    ticks.append((time + 1.0, drain))
    return ticks


def plane_sum(co, axes, mine, slots, send, recv):
    n = 1
    for a in axes:
        n *= DIMS[a]
    me = 0
    for a in axes:
        me = me * DIMS[a] + co[a]
    slots[me] = mine
    copies = []
    for k in range(1, n):
        copy = remote(slots.at[me], slots.at[me], send.at[k], recv.at[0], plane_peer(co, axes, me, k, n))
        copy.start()
        copies.append(copy)
    rest = slots.at[pl.ds(0, n - 1)]
    pltpu.make_async_copy(rest, rest, recv.at[0]).wait()
    for copy in copies:
        copy.wait_send()
    return jnp.sum(slots[...], axis=0)


def plane_peer(co, axes, me, k, n):
    other = lax.rem(me + k, n)
    peer = list(co)
    for a in reversed(axes):
        peer[a] = lax.rem(other, DIMS[a])
        other = lax.div(other, DIMS[a])
    return peer


def plane_peers(co, axes):
    n, me = 1, 0
    for a in axes:
        n *= DIMS[a]
        me = me * DIMS[a] + co[a]
    return [plane_peer(co, axes, me, k, n) for k in range(1, n)]


SUM_PLANES = ((2, 3), (0, 1))


def gather_kernel(layers, rows_ref, down_ref, *rest):
    outs = rest[: 3 * layers]
    got, wide, chunk, xsend, xrecv, sems, local = rest[3 * layers :]
    co = coords()
    size, base, mine = group_peers(co)
    peers = [member(co, base, lax.rem(mine + k, size)) for k in range(1, size)]
    greet(co, peers)
    copies = []
    for k in range(1, size):
        j = lax.rem(mine + k, size)
        copy = remote(rows_ref.at[j], got.at[mine], xsend.at[k], xrecv.at[0], member(co, base, j))
        copy.start()
        copies.append(copy)
    got[pl.ds(mine, 1)] = rows_ref[pl.ds(mine, 1)]
    for l in range(layers):
        chunk[3 * l + 2] = down_ref[l]
    rest_of = got.at[pl.ds(0, size - 1)]
    pltpu.make_async_copy(rest_of, rest_of, xrecv.at[0]).wait()
    per = CH // size
    for l in range(layers):
        for i in range(2):
            row = (2 * l + i) * per
            for t in range(T):
                for j in range(size):
                    wide[t, pl.ds(per * j, per), :] = got[j, t, pl.ds(row, per), :]
            chunk[3 * l + i] = wide[...].astype(bf16)
    for copy in copies:
        copy.wait_send()
    ticks = []
    for l in range(layers):
        for i in range(3):
            n = 3 * l + i
            ticks += gather_ticks(n, outs[n], chunk.at[n], ORDERS[i], co, sems.at[n, 0], sems.at[n, 1], sems.at[n, 2], local.at[n, pl.ds(0, 1)],
                                  local.at[n, pl.ds(1, 1)], start=2.0 * l)
    run(ticks)


def gather(layers, rows, down):
    size = rows.shape[0]
    whole = jax.ShapeDtypeStruct((T,) + DIMS + (CH, CL), bf16)
    return pl.pallas_call(
        functools.partial(gather_kernel, layers),
        out_shape=[whole] * (3 * layers),
        in_specs=[pl.BlockSpec(memory_space=pltpu.VMEM)] * 2,
        out_specs=[pl.BlockSpec(memory_space=pltpu.HBM)] * (3 * layers),
        scratch_shapes=[
            pltpu.VMEM(rows.shape, f32),
            pltpu.VMEM((T, CH, CL), f32),
            pltpu.VMEM((3 * layers, T, CH, CL), bf16),
            pltpu.SemaphoreType.DMA((size,)),
            pltpu.SemaphoreType.DMA((1,)),
            pltpu.SemaphoreType.DMA((3 * layers, 3, 16)),
            pltpu.SemaphoreType.DMA((3 * layers, 2)),
        ],
        compiler_params=pltpu.CompilerParams(collective_id=1, has_side_effects=True, vmem_limit_bytes=30 * 2**20),
        name="gather",
    )(rows, down)


def scatter_kernel(with_total, *refs):
    partials, refs = refs[:3], refs[3:]
    if with_total:
        before, refs = refs[0], refs[1:]
    rows_out, down_out, squares_out, refs = refs[0], refs[1], refs[2], refs[3:]
    scratch, refs = refs[: 3 * SCATTER_SCRATCH], refs[3 * SCATTER_SCRATCH :]
    sums, going, xsend, xrecv = refs[:4]
    co = coords()
    size, base, mine = group_peers(co)
    peers = [member(co, base, lax.rem(mine + k, size)) for k in range(1, size)]
    extra = [p for axes in SUM_PLANES for p in plane_peers(co, axes)] if with_total else []
    greet(co, peers + extra)
    ticks = []
    for i in range(3):
        mine_scratch = scratch[SCATTER_SCRATCH * i : SCATTER_SCRATCH * (i + 1)]
        ticks += scatter_ticks(partials[i], ORDERS[i][::-1], co, mine_scratch, sums.at[i])
    run(ticks)
    down_out[...] = sums[2]
    per = CH // size
    for i in range(2):
        for t in range(T):
            for j in range(size):
                going[j, t, pl.ds(per * i, per), :] = sums[i, t, pl.ds(per * j, per), :]
    copies = []
    for k in range(1, size):
        j = lax.rem(mine + k, size)
        copy = remote(going.at[j], rows_out.at[mine], xsend.at[k], xrecv.at[0], member(co, base, j))
        copy.start()
        copies.append(copy)
    rows_out[pl.ds(mine, 1)] = going[pl.ds(mine, 1)]
    square = sums[...] * sums[...]
    square = jnp.sum(square.reshape(3 * T * CH // 8, 8, CL), axis=0)
    square = square[:, : CL // 2] + square[:, CL // 2 :]
    if with_total:
        square = square + before[...]
        slots_a, slots_b, vsend, vrecv = refs[4:]
        square = plane_sum(co, SUM_PLANES[0], square, slots_a, vsend.at[0], vrecv.at[pl.ds(0, 1)])
        square = plane_sum(co, SUM_PLANES[1], square, slots_b, vsend.at[1], vrecv.at[pl.ds(1, 1)])
        square = jnp.full((8, 128), jnp.sum(square), f32)
    squares_out[...] = square
    rest_of = rows_out.at[pl.ds(0, size - 1)]
    pltpu.make_async_copy(rest_of, rest_of, xrecv.at[0]).wait()
    for copy in copies:
        copy.wait_send()


def scatter(partials, before=None):
    size = min(4, DIMS[2]) * DIMS[3]
    with_total = before is not None
    planes = [DIMS[a] * DIMS[b] for a, b in SUM_PLANES]
    return pl.pallas_call(
        functools.partial(scatter_kernel, with_total),
        out_shape=[
            jax.ShapeDtypeStruct((size, T, -(-2 * (CH // size) // 8) * 8, CL), f32),
            jax.ShapeDtypeStruct((T, CH, CL), f32),
            jax.ShapeDtypeStruct((8, 128), f32),
        ],
        in_specs=[pl.BlockSpec(memory_space=pltpu.HBM)] * 3 + [pl.BlockSpec(memory_space=pltpu.VMEM)] * with_total,
        out_specs=[pl.BlockSpec(memory_space=pltpu.VMEM)] * 3,
        scratch_shapes=[s for i in range(3) for s in scatter_scratch(ORDERS[i][::-1])]
        + [
            pltpu.VMEM((3, T, CH, CL), f32),
            pltpu.VMEM((size, T, -(-2 * (CH // size) // 8) * 8, CL), f32),
            pltpu.SemaphoreType.DMA((size,)),
            pltpu.SemaphoreType.DMA((1,)),
        ]
        + [
            pltpu.VMEM((planes[0], 8, 128), f32),
            pltpu.VMEM((planes[1], 8, 128), f32),
            pltpu.SemaphoreType.DMA((2, max(planes))),
            pltpu.SemaphoreType.DMA((2,)),
        ]
        * with_total,
        compiler_params=pltpu.CompilerParams(collective_id=3 if with_total else 2, has_side_effects=True, vmem_limit_bytes=62 * 2**20),
        name="scatter",
    )(*partials, *([before] if with_total else []))

FB = 512
NJ = FB // CL
RC = 256
EPS = 1e-6


def dot(a, b):
    return jnp.dot(a, b, preferred_element_type=f32)


def dot_nt(a, b):
    return lax.dot_general(a, b, (((1,), (1,)), ((), ())), preferred_element_type=f32)


def block_of(ref, j):
    return ref[0, :, j].reshape(-1, CL)


def parts(gate, up, dhid):
    s = jax.nn.sigmoid(gate)
    silu = gate * s
    wide = dhid.astype(bf16).astype(f32)
    hid = (silu * up).astype(bf16)
    dup = (wide * silu).astype(bf16)
    dgate = (wide * up * (s + silu * (1.0 - s))).astype(bf16)
    return hid, dup, dgate


def dhid_of(dh, wd_ref, j):
    return sum(dot_nt(dh[:, t * CL : (t + 1) * CL], wd_ref[t, pl.ds(j * CL, CL), :]) for t in range(T))


def rows_of(i, n=RC):
    return pl.ds(pl.multiple_of(i * n, n), n)


def normed(h):
    wide = h.astype(f32)
    scale = lax.rsqrt(jnp.mean(wide**2, -1, keepdims=True) + EPS)
    return (wide * scale).astype(bf16)


def weight_gradients(at_ref, dh_ref, dgate, dup, hid_t, pg_ref, pu_ref, pd_ref):
    d = at_ref.shape[0]
    mc = 16 * CH
    for src, dst in ((dgate, pg_ref), (dup, pu_ref)):
        for m in range(d // mc):
            for j in range(NJ):
                value = dot(at_ref[pl.ds(m * mc, mc), :], src[:, pl.ds(j * CL, CL)])
                dst[0, pl.ds(m * 16, 16), j] = value.reshape(16, CH, CL).astype(bf16)
    for j in range(NJ):
        value = dot(hid_t[pl.ds(j * CL, CL), :], dh_ref[...]).astype(bf16)
        for t in range(T):
            pd_ref[t, pl.ds(j * CL, CL), :] = value[:, t * CL : (t + 1) * CL]


def first_kernel(x_ref, wg_ref, wu_ref, wd_ref, gate_ref, up_ref, at_ref, h_ref, a2_ref, a2t_ref, a_s, y_s):
    b = pl.program_id(0)
    n = x_ref.shape[0] // RC

    @pl.when(b == 0)
    def _():
        for i in range(n):
            r = pl.ds(i * RC, RC)
            a = normed(x_ref[r, :])
            a_s[r, :] = a
            at_ref[:, r] = a.T
        y_s[...] = jnp.zeros_like(y_s)

    def chunk(i, _):
        r = rows_of(i)
        hids = []
        for j in range(NJ):
            c = pl.ds(j * CL, CL)
            gate = dot(a_s[r, :], block_of(wg_ref, j))
            up = dot(a_s[r, :], block_of(wu_ref, j))
            gate_ref[0, r, c] = gate
            up_ref[0, r, c] = up
            hids.append((gate * jax.nn.sigmoid(gate) * up).astype(bf16))
        hid = jnp.concatenate(hids, axis=1)
        for t in range(T):
            c = pl.ds(t * CL, CL)
            y_s[r, c] += dot(hid, wd_ref[t])
        return 0

    lax.fori_loop(0, n, chunk, 0)

    @pl.when(b == pl.num_programs(0) - 1)
    def _():
        for i in range(n):
            r = pl.ds(i * RC, RC)
            h = x_ref[r, :] + y_s[r, :].astype(bf16)
            h_ref[r, :] = h
            a2 = normed(h)
            a2_ref[r, :] = a2
            a2t_ref[:, r] = a2.T


def weight_spec():
    nt = 8 // NJ
    return pl.BlockSpec((1, 32, NJ, CH, CL), lambda b: (b // nt, 0, b % nt, 0, 0))


def down_spec():
    return pl.BlockSpec((T, FB, CL), lambda b: (0, b, 0))


def whole(shape):
    return pl.BlockSpec(shape, lambda b: (0,) * len(shape))


PARAMS = dict(vmem_limit_bytes=60 * 2**20, dimension_semantics=("arbitrary",))


def cost(matmuls, bytes_accessed):
    return pl.CostEstimate(flops=matmuls * 2 * 1024 * 768 * 6144, bytes_accessed=bytes_accessed, transcendentals=1024 * 6144)


def first(x, wg, wu, wd):
    tokens, d = x.shape
    ff = wd.shape[1]
    nb = ff // FB
    return pl.pallas_call(
        first_kernel,
        grid=(nb,),
        in_specs=[whole((tokens, d)), weight_spec(), weight_spec(), down_spec()],
        out_specs=[
            pl.BlockSpec((1, tokens, FB), lambda b: (b, 0, 0)),
            pl.BlockSpec((1, tokens, FB), lambda b: (b, 0, 0)),
            whole((d, tokens)),
            whole((tokens, d)),
            whole((tokens, d)),
            whole((d, tokens)),
        ],
        out_shape=[
            jax.ShapeDtypeStruct((nb, tokens, FB), f32),
            jax.ShapeDtypeStruct((nb, tokens, FB), f32),
            jax.ShapeDtypeStruct((d, tokens), bf16),
            jax.ShapeDtypeStruct((tokens, d), bf16),
            jax.ShapeDtypeStruct((tokens, d), bf16),
            jax.ShapeDtypeStruct((d, tokens), bf16),
        ],
        scratch_shapes=[pltpu.VMEM((tokens, d), bf16), pltpu.VMEM((tokens, d), f32)],
        compiler_params=pltpu.CompilerParams(**PARAMS),
        cost_estimate=cost(3, 80 * 2**20),
        name="first_layer",
    )(x, wg, wu, wd)


def second_kernel(a_ref, at_ref, h_ref, dy_ref, wg_ref, wu_ref, wd_ref, pg_ref, pu_ref, pd_ref, dh_ref, da_s, dgate_s, dup_s, hid_t):
    b = pl.program_id(0)
    n = a_ref.shape[0] // RC

    @pl.when(b == 0)
    def _():
        da_s[...] = jnp.zeros_like(da_s)

    def chunk(i, _):
        r = rows_of(i)
        a = a_ref[r, :]
        dy = dy_ref[r, :]
        da = da_s[r, :]
        for j in range(NJ):
            c = pl.ds(j * CL, CL)
            wg, wu = block_of(wg_ref, j), block_of(wu_ref, j)
            hid, dup, dgate = parts(dot(a, wg), dot(a, wu), dhid_of(dy, wd_ref, j))
            dgate_s[r, c] = dgate
            dup_s[r, c] = dup
            hid_t[c, r] = hid.T
            da += dot_nt(dgate, wg) + dot_nt(dup, wu)
        da_s[r, :] = da
        return 0

    lax.fori_loop(0, n, chunk, 0)
    weight_gradients(at_ref, dy_ref, dgate_s, dup_s, hid_t, pg_ref, pu_ref, pd_ref)

    @pl.when(b == pl.num_programs(0) - 1)
    def _():
        for i in range(n):
            r = pl.ds(i * RC, RC)
            wide = h_ref[r, :].astype(f32)
            da = da_s[r, :].astype(bf16).astype(f32)
            scale = lax.rsqrt(jnp.mean(wide**2, -1, keepdims=True) + EPS)
            inner = jnp.mean(da * wide, -1, keepdims=True)
            dh = da * scale - wide * (inner * scale * scale * scale)
            dh_ref[r, :] = dy_ref[r, :] + dh.astype(bf16)


def second(a, at, h, dy, wg, wu, wd):
    tokens, d = a.shape
    ff = wd.shape[1]
    return pl.pallas_call(
        second_kernel,
        grid=(ff // FB,),
        in_specs=[whole((tokens, d)), whole((d, tokens)), whole((tokens, d)), whole((tokens, d)), weight_spec(), weight_spec(), down_spec()],
        out_specs=[weight_spec(), weight_spec(), down_spec(), whole((tokens, d))],
        out_shape=[
            jax.ShapeDtypeStruct(wg.shape, bf16),
            jax.ShapeDtypeStruct(wg.shape, bf16),
            jax.ShapeDtypeStruct(wd.shape, bf16),
            jax.ShapeDtypeStruct((tokens, d), bf16),
        ],
        scratch_shapes=[pltpu.VMEM((tokens, d), f32), pltpu.VMEM((tokens, FB), bf16), pltpu.VMEM((tokens, FB), bf16), pltpu.VMEM((FB, tokens), bf16)],
        compiler_params=pltpu.CompilerParams(**PARAMS),
        cost_estimate=cost(8, 60 * 2**20),
        name="second_layer",
    )(a, at, h, dy, wg, wu, wd)


def third_kernel(gate_ref, up_ref, at_ref, dh_ref, wd_ref, pg_ref, pu_ref, pd_ref, dgate_s, dup_s, hid_t):
    n = dh_ref.shape[0] // RC

    def chunk(i, _):
        r = rows_of(i)
        dh = dh_ref[r, :]
        for j in range(NJ):
            c = pl.ds(j * CL, CL)
            hid, dup, dgate = parts(gate_ref[0, r, c], up_ref[0, r, c], dhid_of(dh, wd_ref, j))
            dgate_s[r, c] = dgate
            dup_s[r, c] = dup
            hid_t[c, r] = hid.T
        return 0

    lax.fori_loop(0, n, chunk, 0)
    weight_gradients(at_ref, dh_ref, dgate_s, dup_s, hid_t, pg_ref, pu_ref, pd_ref)


def third(gate, up, at, dh, wd, like):
    tokens, d = dh.shape
    ff = wd.shape[1]
    return pl.pallas_call(
        third_kernel,
        grid=(ff // FB,),
        in_specs=[
            pl.BlockSpec((1, tokens, FB), lambda b: (b, 0, 0)),
            pl.BlockSpec((1, tokens, FB), lambda b: (b, 0, 0)),
            whole((d, tokens)),
            whole((tokens, d)),
            down_spec(),
        ],
        out_specs=[weight_spec(), weight_spec(), down_spec()],
        out_shape=[jax.ShapeDtypeStruct(like.shape, bf16), jax.ShapeDtypeStruct(like.shape, bf16), jax.ShapeDtypeStruct(wd.shape, bf16)],
        scratch_shapes=[pltpu.VMEM((tokens, FB), bf16), pltpu.VMEM((tokens, FB), bf16), pltpu.VMEM((FB, tokens), bf16)],
        compiler_params=pltpu.CompilerParams(**PARAMS),
        cost_estimate=cost(4, 90 * 2**20),
        name="first_layer_back",
    )(gate, up, at, dh, wd)


def adamw(w, m, v, g):
    m = 0.9 * m + 0.1 * g
    v = 0.95 * v + 0.05 * g * g
    step = m * lax.rsqrt(v + 1e-8) + 0.1 * w
    return (w - 0.02 * step).astype(bf16), m, v


def solution(mesh):
    def step(x, dy, w_gate, w_up, w_down, *moments):
        m, v = moments[:3], moments[3:]
        weights = (w_gate, w_up, w_down)
        layers, per, ff = w_gate.shape
        size = CH // per
        rows = jnp.stack([w_gate, w_up], 1).astype(f32).reshape(layers, 2, per, T, size, CL).transpose(4, 3, 0, 1, 2, 5)
        rows = rows.reshape(size, T, layers * 2 * per, CL)
        rows = jnp.pad(rows, ((0, 0), (0, 0), (0, -rows.shape[2] % 8), (0, 0)))
        down = w_down.reshape(layers, CH, T, CL).transpose(0, 2, 1, 3)
        full = gather(layers, rows, down)
        blocks = (T, 32, 8, CH, CL)
        shapes = (blocks, blocks, (T, 256 * CH, CL))
        first_w, second_w = ([a.reshape(s) for a, s in zip(full[3 * l : 3 * l + 3], shapes)] for l in range(2))
        gate, up, a1t, h1, a2, a2t = first(x[0], *first_w)
        *partial2, dh1 = second(a2, a2t, h1, dy[0], *second_w)
        partial1 = third(gate, up, a1t, dh1, first_w[2], first_w[0])
        cut = (T,) + DIMS + (CH, CL)
        rows2, down2, square2 = scatter([p.reshape(cut) for p in partial2])
        rows1, down1, total = scatter([p.reshape(cut) for p in partial1], square2)

        def rows_of_gradient(got, i):
            return got[:, :, per * i : per * i + per].transpose(2, 1, 0, 3).reshape(per, ff)

        gradients = [jnp.stack([rows_of_gradient(r, i) for r in (rows1, rows2)]) for i in range(2)]
        gradients.append(jnp.stack([d.transpose(1, 0, 2).reshape(CH, T * CL) for d in (down1, down2)]))
        count = 256 * sum(w.size for w in weights)
        factor = jnp.minimum(1.0, 0.5 * lax.rsqrt(total[0, 0] / count + 1e-30))
        new = [adamw(w.astype(f32), m, v, g * factor) for w, m, v, g in zip(weights, m, v, gradients, strict=True)]
        return tuple(one[which] for which in range(3) for one in new)

    states, cut = P(("rep", "dp"), None, None), P(None, "dp", None)
    return jax.shard_map(
        step,
        mesh=mesh,
        in_specs=(states, states) + (cut,) * 9,
        out_specs=(P("rep", "dp", None),) * 9,
        check_vma=False,
    )
```

```python
import functools
import jax
import jax.numpy as jnp
from jax import lax
from jax.experimental import pallas as pl
from jax.experimental.pallas import tpu as pltpu
from jax.sharding import PartitionSpec as P

DIMS = (4, 4, 8, 2)
T = 3
CH, CL, DR, D = 24, 256, 8, 768
CHUNK, PIECE = (CH, CL), (DR, D)
SHAPES = (CHUNK, CHUNK, PIECE)
XYZ = DIMS[:3]
SIZE, PER = 8, 3
ORDERS = ((0, 1, 2), (2, 1, 0), (2, 0, 1))
MATS = range(len(ORDERS))
WAYS = (1, -1)
BOTH = range(2)
f32, bf16 = jnp.float32, jnp.bfloat16
ALL = slice(None)
LANES = CL // 2
LINK = CH * CL * 2 / 46.6e3
HOP = 3.3


def apart(n):
    return range(1, n)


def part(half):
    return 0.5 if half else 1.0


def flat(co):
    r = co[0]
    for n, i in zip(DIMS[1:], co[1:]):
        r = r * n + i
    return r


class Here(list):
    def __init__(self):
        r = lax.axis_index("dp")
        self.index = r
        for n in DIMS[::-1]:
            self.insert(0, lax.rem(r, n))
            r = lax.div(r, n)
        self.pos, self.dev = [], []
        for axis, n in enumerate(DIMS):
            self.pos.append([self[axis]] + [lax.rem(self[axis] + k, n) for k in apart(n)])
            self.dev.append([flat(self[:axis] + [p] + self[axis + 1 :]) for p in self.pos[axis]])
        self.partner = self.dev[3][1]
        half = SIZE // 2
        z = lax.rem(self[2], half)
        base = self.index - z * 2 - self[3]
        self.mine = z * 2 + self[3]
        self.group = [(j, base + j) for j in (lax.rem(self.mine + k, SIZE) for k in apart(SIZE))]


def place(co, axis, by):
    return co.pos[axis][by % DIMS[axis]]


def peer(co, axis, by):
    return co.dev[axis][by % DIMS[axis]]


def axis_peers(co):
    return [co.dev[a][k] for a in MATS for k in apart(DIMS[a])]


def plane_peers(co, axes):
    (i, m), (j, n) = ((co[a], DIMS[a]) for a in axes)
    strides = [flat([int(a == b) for b in range(len(DIMS))]) for a in axes]
    me = i * n + j
    base = co.index - i * strides[0] - j * strides[1]
    others = [lax.rem(me + k, m * n) for k in apart(m * n)]
    return me, [base + lax.div(o, n) * strides[0] + lax.rem(o, n) * strides[1] for o in others]


PLANES = ((2, 3), (0, 1))


def greet(peers):
    barrier = pltpu.get_barrier_semaphore()
    for peer in peers:
        pl.semaphore_signal(barrier, inc=1, device_id={"dp": peer})
    pl.semaphore_wait(barrier, len(peers))


def remote(src, dst, ssem, rsem, device):
    return pltpu.make_async_remote_copy(src_ref=src, dst_ref=dst, send_sem=ssem, recv_sem=rsem, device_id={"dp": device})


def loop(n, body, lo=0):
    def step(i, _):
        body(i)
        return 0

    lax.fori_loop(lo, lo + n, step, 0)


def await_bytes(view, sem):
    pltpu.make_async_copy(view, view, sem).wait()


def upto(n):
    return pl.ds(0, n)


def side(by):
    return (1 - by) // 2


def cut(n, half):
    return ALL if half is ALL else pl.ds(half * (n // 2), n // 2)


(KEEP, SWAP_SEND, SWAP_RECV, RING_SEND, SEND1, RECV1, SEND2, RECV2, SEND3, RECV3), RING_RECV = range(10), 8
SEMS = 18


def far(n):
    return n * n / 8


class Stream:
    def __init__(self, after=()):
        self.ticks, self.after, self.next, self.ready, self.marks = [], after, 0, 0.0, {}

    def add(self, run, axis=-1, load=0.0, travel=0.0, after=()):
        self.ticks.append((run, axis, load, travel, after))

    def mark(self, name):
        self.marks[name] = len(self.ticks)

    def passed(self, name):
        return self.next >= self.marks[name]


def at(ref, sel, core=ALL):
    index = list(sel) + ([] if core is ALL else [core])
    return ref.at[tuple(index)]


def gather_stream(ref, own, order, co, sems, after=()):
    s = Stream(after)
    c = co[3]
    a1, a2, a3 = order
    n1, n2, n3 = (DIMS[a] for a in order)

    def sel(i, j, k):
        out = [0, 0, 0]
        out[a1], out[a2], out[a3] = i, j, k
        return out

    mine = at(ref, co[:3], c)
    keep = lambda: pltpu.make_async_copy(own, mine, sems.at[KEEP])
    block2 = lambda: at(ref, sel(ALL, co[a2], co[a3]), c)

    def block3(k, half=ALL):
        return at(ref, sel(cut(n1, half), ALL, k), c)

    def forward(view):
        remote(view, view, sems.at[SWAP_SEND], sems.at[SWAP_RECV], co.partner).start()

    def spread(source, target, n, axis, i, j):
        for k in apart(n):
            remote(source, target, sems.at[i], sems.at[j], peer(co, axis, k)).start()

    def one():
        keep().start()
        spread(own, mine, n1, a1, SEND1, RECV1)

    def two():
        await_bytes(at(ref, sel(upto(n1 - 1), 0, 0), c), sems.at[RECV1])
        keep().wait()
        spread(block2(), block2(), n2, a2, SEND2, RECV2)

    def ring(step, by):
        half = side(by) if step == n3 // 2 else ALL
        view = block3(place(co, a3, -by * (step - 1)), half)
        came = block3(place(co, a3, -by * step), half)
        return remote(view, view, sems.at[RING_SEND], sems.at[RING_RECV + 2 * step + side(by)], peer(co, a3, by)), came

    def three(step):
        if step == 1:
            await_bytes(at(ref, sel(ALL, upto(n2 - 1), 0), c), sems.at[RECV2])
        for by in WAYS:
            if step > 1:
                ring(step - 1, by)[0].wait_recv()
            if step <= n3 // 2:
                ring(step, by)[0].start()
        if step == 1:
            forward(block3(co[a3]))
        else:
            for by in WAYS:
                forward(ring(step - 1, by)[1])

    def finish():
        half = at(ref, [ALL] * 3, 1 - c)
        await_bytes(half, sems.at[SWAP_RECV])

    def drain():
        half = at(ref, [ALL] * 3, c)
        await_bytes(half, sems.at[SWAP_SEND])
        await_bytes(at(ref, sel(upto(n1 - 1), 0, 0), c), sems.at[SEND1])
        await_bytes(at(ref, sel(ALL, upto(n2 - 1), 0), c), sems.at[SEND2])
        await_bytes(at(ref, sel(ALL, ALL, upto(n3 - 1)), c), sems.at[RING_SEND])

    s.add(one, a1, far(n1) * LINK, HOP + n1 / 8)
    s.add(two, a2, far(n2) * n1 * LINK, HOP + n2 / 8)
    for step in range(1, n3 // 2 + 1):
        s.add(functools.partial(three, step), a3, n1 * n2 * LINK * part(step == n3 // 2), HOP)
    s.add(functools.partial(three, n3 // 2 + 1), travel=2.0)
    s.add(finish)
    s.mark("done")
    s.add(drain)
    s.mark("end")
    return s


def swap_block(partial, other, m, b, co, sems):
    for half in range(2 if m < 2 else 1):
        index = (ALL, ALL, half * 4 + b) if m < 2 else (b,)
        remote(partial.at[index], other.at[index], sems.at[SWAP_SEND], sems.at[SWAP_RECV], co.partner).start()


def scatter_scratch(deep):
    out = []
    for order, shape in zip(ORDERS, SHAPES):
        n2, n3 = DIMS[order[1]], DIMS[order[0]]
        out += [
            pltpu.VMEM((deep,) + XYZ + shape, bf16),
            pltpu.VMEM((deep,) + XYZ + shape, bf16),
            pltpu.VMEM((n3,) + shape, f32),
            pltpu.VMEM((n2, n3) + shape, bf16),
            pltpu.VMEM((2, n2 - 1, n3) + shape, bf16),
            pltpu.VMEM((2, n3 - 1) + shape, bf16),
            pltpu.SemaphoreType.DMA((T + 1, SEMS)),
            pltpu.SemaphoreType.REGULAR((len(WAYS) + 1,)),
        ]
    return out


SCRATCH = 8


def scatter_stream(kept, order, co, scratch, out, stage, swapped, swaps, rings, before):
    other, came1, total, going, came2, came3, sems, free = scratch
    deep = other.shape[0]
    other, came1 = other.at[stage % deep], came1.at[stage % deep]
    came2, came3, sems = came2.at[stage % 2], came3.at[stage % 2], sems.at[stage]
    s = Stream()
    b3, b2, b1 = order
    n1, n2, n3 = (DIMS[a] for a in (b1, b2, b3))
    p1, p2, p3 = (co[a] for a in (b1, b2, b3))
    mid = n1 // 2

    def sel(q, i=ALL, j=ALL):
        out = [0, 0, 0]
        out[b1], out[b2], out[b3] = q, i, j
        return out

    def chunk_sum(refs, q, i):
        return sum(r[tuple(sel(q, i))].astype(f32) for r in refs)

    def sums(q, lo, size, refs):
        def body(i):
            kept[tuple(sel(q, i))] = chunk_sum(refs, q, i).astype(bf16)

        loop(size, body, lo)

    def ring(step, by):
        q = place(co, b1, by * (mid + 1 - step))
        slot = place(co, b1, mid - 1) if by < 0 and step == mid else q
        half = side(by) if step == 1 else ALL
        view, target = at(kept, sel(q, cut(n2, half))), at(came1, sel(slot, cut(n2, half)))
        return remote(view, target, sems.at[RING_SEND], sems.at[RING_RECV + 2 * step + side(by)], peer(co, b1, by))

    def around(step):
        if step == 1 and swapped:
            await_bytes(other, sems.at[SWAP_RECV])
            await_bytes(other, sems.at[SWAP_SEND])
        for by in WAYS:
            q = place(co, b1, by * (mid + 1 - step))
            if step == 1:
                if stage >= deep:
                    pl.semaphore_wait(free.at[1 + side(by)], 1)
                sums(q, side(by) * (n2 // 2), n2 // 2, (kept, other))
            else:
                ring(step - 1, by).wait_recv()
                if step == 2:
                    sums(q, side(by) * (n2 // 2), n2 // 2, (kept, other, came1))
                    sums(q, side(-by) * (n2 // 2), n2 // 2, (kept, other))
                else:
                    sums(q, 0, n2, (kept, other, came1))
            ring(step, by).start()

    def middle():
        for by in WAYS:
            ring(mid, by).wait_recv()
        opposite = place(co, b1, mid)

        def value(i):
            return chunk_sum((kept, other, came1), p1, i) + came1[tuple(sel(opposite, i))].astype(f32)

        def body(i):
            going[i] = value(i).astype(bf16)

        loop(n2, body)
        total[...] = value(p2)
        for k in apart(n2):
            remote(going.at[place(co, b2, k)], came2.at[k - 1], sems.at[SEND2], sems.at[RECV2], peer(co, b2, k)).start()
        if stage + deep < rings:
            for by in WAYS:
                pl.semaphore_signal(free.at[1 + side(-by)], inc=1, device_id={"dp": peer(co, b1, by)})
        if stage + deep < swaps:
            pl.semaphore_signal(free.at[0], inc=1, device_id={"dp": co.partner})

    def release():
        await_bytes(at(came1, sel(upto(n1 - 1))), sems.at[RING_SEND])

    def late():
        await_bytes(came2, sems.at[RECV2])
        await_bytes(came2, sems.at[SEND2])
        value = total[...] + jnp.sum(came2[...].astype(f32), axis=0)
        total[...] = value
        going[p2] = value.astype(bf16)
        for k in apart(n3):
            remote(going.at[p2, place(co, b3, k)], came3.at[k - 1], sems.at[SEND3], sems.at[RECV3], peer(co, b3, k)).start()

    def last():
        await_bytes(came3, sems.at[RECV3])
        value = total[p3] + jnp.sum(came3[...].astype(f32), axis=0)
        out[...] = value.astype(bf16).astype(f32)
        await_bytes(came3, sems.at[SEND3])

    for step in range(1, mid + 1):
        s.add(functools.partial(around, step), b1, n2 * n3 * LINK * part(step == 1), HOP + 0.7)
        s.marks.setdefault("begun", len(s.ticks))
    s.add(middle, b2, far(n2) * n3 * LINK, HOP + n2 / 8, [(p, "end") for p in before])
    s.mark("middle")
    s.add(release)
    s.mark("free")
    s.add(late, b3, far(n3) * LINK, HOP + n3 / 8)
    s.add(last)
    s.mark("end")
    return s


class Plan:
    def __init__(self, streams):
        self.streams, self.busy, self.now, self.slots, self.done = streams, [0.0] * 4, 0.0, [], {}

    def open(self, s):
        return s.next < len(s.ticks) and all(other.passed(name) for other, name in (*s.after, *s.ticks[s.next][-1]))

    def run(self, s):
        run, axis, load, travel, _ = s.ticks[s.next]
        self.slots[-1].append(run)
        begin = max(self.now, self.busy[axis])
        if load:
            self.busy[axis] = begin + load
        s.next += 1
        s.ready = begin + load + travel

    def slot(self, length=0.0):
        self.slots.append([])
        more = True
        while more:
            more = False
            for s in self.streams:
                if self.open(s) and s.ready <= self.now:
                    self.run(s)
                    more = True
        self.now += length

    def need(self, wanted):
        while not all(s.passed(name) for s, name in wanted):
            s = min((s for s in self.streams if self.open(s)), key=lambda s: s.ready)
            self.now = max(self.now, s.ready)
            self.run(s)

    def take(self):
        out, self.slots = self.slots, []
        return out


def run_slot(slots, index, fold=8):
    for lo in range(0, len(slots), fold):
        some = slots[lo : lo + fold]
        if any(some):

            def inner(lo=lo, some=some):
                for i, ticks in enumerate(some):
                    if ticks:

                        @pl.when(index == lo + i)
                        def _(ticks=ticks):
                            for tick in ticks:
                                tick()

            pl.when(lax.div(index, fold) == lo // fold)(inner)

TOKENS = 1024
FB = 512
NJ = FB // CL
NB = 4
RC = 512
NC = TOKENS // RC
END = NC - 1
EPS = 1e-6
NORM = 128
LAST = T * NB - 1
WIDE = (2, 4, 4, 2, 2) + CHUNK


def dot(a, b):
    return jnp.dot(a, b, preferred_element_type=f32)


def dot_nt(a, b):
    return lax.dot_general(a, b, (((1,), (1,)), ((), ())), preferred_element_type=f32)


def odd(b):
    return lax.rem(b, 2)


def rows_of(i, n=RC):
    return pl.ds(pl.multiple_of(i * n, n), n)


def over_rows(body):
    loop(TOKENS // NORM, lambda i: body(rows_of(i, NORM)))


def normed(h):
    wide = h.astype(f32)
    scale = lax.rsqrt(jnp.mean(wide**2, -1, keepdims=True) + EPS)
    return (wide * scale).astype(bf16)


def fetch(refs, b, w, wd, sems):
    out = []
    for m in MATS:
        if m in refs:
            ref = refs[m]
            if m < 2:
                for half in BOTH:
                    out.append(pltpu.make_async_copy(ref.at[:, :, half * 4 + b], w.at[m, :, :, half], sems.at[m, half]))
            else:
                out.append(pltpu.make_async_copy(ref.at[b], wd, sems.at[m, 0]))
    return out


def rows_of_down(wd, j):
    return wd[pl.ds(2 * j, 2)].reshape(CL, D)


def columns_of(w, m, j):
    return w[m, :, :, :, j].reshape(D, CL)


def pieces(device):
    return [(lax.rem(T * device + i, DEVICES), lax.div(T * device + i, DEVICES)) for i in range(T)]


def origins(device):
    return [(lax.div(DEVICES * t + device, T), lax.rem(DEVICES * t + device, T)) for t in range(T)]


def piece_peers(here):
    return [d for d, _ in pieces(here) + origins(here)]


def routes(out, here):
    return [(i, *to) for i, to in enumerate(pieces(here) if out else origins(here))]


def start_pieces(src, dst, here, sems, out):
    for i, device, slot in routes(out, here):

        @pl.when(device != here)
        def _(i=i, device=device, slot=slot):
            remote(src.at[i], dst.at[slot], sems.at[i], sems.at[T + slot], device).start()

        @pl.when(device == here)
        def _(i=i, slot=slot):
            dst[slot] = src[i]


def await_pieces(src, dst, here, sems, out):
    for i, device, _ in routes(out, here):

        @pl.when(device != here)
        def _(i=i):
            await_bytes(src.at[i], sems.at[i])

    for i, device, _ in routes(not out, here):

        @pl.when(device != here)
        def _(i=i):
            await_bytes(dst.at[i], sems.at[T + i])


def parts(gate, up, dhid):
    s = jax.nn.sigmoid(gate)
    silu = gate * s
    wide = dhid.astype(bf16).astype(f32)
    hid = (silu * up).astype(bf16)
    dup = (wide * silu).astype(bf16)
    dgate = (wide * up * (s + silu * (1.0 - s))).astype(bf16)
    return hid, dup, dgate


def weight_gradients(at_s, dh_s, dgate, dup, hid_t, wide, down, slots, b):
    half = D // 2
    for m, src in enumerate((dgate, dup)):
        for i in BOTH:
            for j in range(NJ):
                value = dot(at_s[pl.ds(i * half, half), :], src[:, pl.ds(j * CL, CL)]).reshape((2, 4, 2) + CHUNK).astype(bf16)
                for z in BOTH:
                    wide[slots[j], m, pl.ds(2 * i, 2), :, z * 4 + b] = value[:, :, z]
    for j in range(NJ):
        value = dot(hid_t[pl.ds(j * CL, CL), :], dh_s[...]).reshape((2, 8, 2) + PIECE).astype(bf16)
        for c in BOTH:
            down[slots[c], b, pl.ds(2 * j, 2)] = value[:, :, c]


def gradients_step(co, tensors, buffers, scratch, stage, b, deep):
    wide_s, down_s = buffers
    slot = lax.rem(stage, deep)
    slots = [slot * me + deep * (1 - me) for me in (1 - co[3], co[3])]
    weight_gradients(*tensors, wide_s, down_s, slots, b)

    @pl.when(stage >= deep)
    def _():
        @pl.when(b == 0)
        def _():
            for m in MATS:
                pl.semaphore_wait(scratch[m][SCRATCH - 1].at[0], 1)

    for m in MATS:
        swap_block(wide_s.at[deep, m] if m < 2 else down_s.at[deep], scratch[m][0].at[slot], m, b, co, scratch[m][SCRATCH - 2].at[stage])


def scatter_stage(plan, scatters, co, buffers, scratch, sums, swapped, swaps, rings, deep, start):
    n = len(scatters)
    stage = []
    for m in MATS:
        before = [scatters[n - 1][m]] if n else []
        kept = buffers[0].at[n % deep, m] if m < 2 else buffers[1].at[n % deep]
        stage.append(scatter_stream(kept, ORDERS[m], co, scratch[m], sums(n, m), n, swapped, swaps, rings, before))
        stage[m].ready = start
    scatters.append(stage)
    plan.streams += stage


def forward_kernel(rows_ref, down_ref, x_ref, dy_ref, *refs):
    full, refs = (refs[:3], refs[3:6]), refs[6:]
    gate_ref, up_ref, at_ref, dh_ref, wide_kept, down_kept, *refs = refs
    other_kept, refs = refs[:3], refs[3:]
    sums, dsums, *refs = refs
    scratch = [refs[SCRATCH * m : SCRATCH * (m + 1)] for m in MATS]
    got, wide, chunks, eights, a_s, at_s, h_s, dh_s, acc, dgate_s, dup_s, hid_t, w, wd, held, wide_s, down_s, *refs = refs[SCRATCH * 3 :]
    gsems, wsems, hsems, lsems, xsems, dsems = refs
    co = Here()
    mine, here = co.mine, co.index
    greet(axis_peers(co) + [co.partner] + [device for _, device in co.group] + piece_peers(here))

    stages = 2 * T
    rest = pl.ds(1, stages - 1)

    def swap(j, device, part, i):
        return remote(rows_ref.at[j, part], got.at[mine, part], xsems.at[i], xsems.at[i + 1], device)

    for part, i in ((0, 0), (rest, 2)):
        for j, device in co.group:
            swap(j, device, part, i).start()
        if i == 0:
            start_pieces(down_ref, eights, here, dsems, True)
    loads = [pltpu.make_async_copy(src, dst, lsems.at[i]) for i, (src, dst) in enumerate(((x_ref, h_s), (dy_ref, dh_s)))]
    for copy in loads:
        copy.start()
    got[pl.ds(mine, 1)] = rows_ref[pl.ds(mine, 1)]
    others = got.at[upto(SIZE - 1)]

    def own(n):
        for m in BOTH:
            for j in range(SIZE):
                wide[pl.ds(PER * j, PER), :] = got[j, n, pl.ds(m * PER, PER), :]
            chunks[n, m] = wide[...].astype(bf16)

    await_bytes(others.at[:, 0], xsems.at[1])
    own(0)
    await_pieces(down_ref, eights, here, dsems, True)
    gathers, scatters = [], []
    for n in range(stages):
        after = [(s, "begin") for s in gathers[n - 1]] if n else []
        l, t = n // T, n % T
        stage = [gather_stream(full[l][m].at[t], chunks.at[n, m] if m < 2 else eights.at[t, l], ORDERS[m], co, gsems.at[n, m], after) for m in MATS]
        for s in stage:
            s.marks["begin"] = BEGIN
        gathers.append(stage)
    plan = Plan([s for stage in gathers for s in stage])

    def now():
        for ticks in plan.take():
            for tick in ticks:
                tick()

    def start_scatter():
        scatter_stage(plan, scatters, co, (wide_s, down_s), scratch, lambda n, m: sums.at[n, m] if m < 2 else dsums.at[n], True, T, DEEP, DEEP, plan.now + SETTLE)

    plan.slot(6.0)
    now()
    for copy in loads:
        copy.wait()

    def norm(r):
        a = normed(h_s[r, :])
        a_s[r, :] = a
        at_s[:, r] = a.T
        acc[r, :] = jnp.zeros((NORM, D), f32)

    over_rows(norm)
    put_at = pltpu.make_async_copy(at_s, at_ref, lsems.at[0])
    put_at.start()
    await_bytes(others.at[:, rest], xsems.at[3])
    for n in range(1, stages):
        own(n)
    plan.slot()
    plan.need([(s, "done") for s in gathers[0]])
    now()

    def weights(layer, t, b):
        return fetch(dict(enumerate(ref.at[t] for ref in full[layer])), lax.rem(b, NB), w.at[odd(b)], wd.at[odd(b)], wsems.at[odd(b)])

    def fetch_next(layer, b):
        for copy in weights(layer, lax.div(b, NB), b):
            copy.start()

    def await_block(b):
        for copy in weights(0, 0, b):
            copy.wait()

    fetch_next(0, 0)
    blocks = T * NB
    for b in range(blocks):
        for i in range(NC):
            plan.slot(FIRST_US)
            if i == END and b % NB == NB - 1 and b < LAST:
                plan.need([(s, "done") for s in gathers[b // NB + 1]])
    slots1 = plan.take()

    def put(b, i):
        return [pltpu.make_async_copy(held.at[i, k], ref.at[b, i], hsems.at[i, k]) for k, ref in enumerate((gate_ref, up_ref))]

    def block1(b):
        await_block(b)
        now_w, now_wd = w.at[odd(b)], wd.at[odd(b)]

        def chunk(i):
            run_slot(slots1, b * NC + i)

            @pl.when(b < LAST)
            def _():
                @pl.when(i == lax.div(lax.rem(b, NB), NB - 1) * (END))
                def _():
                    fetch_next(0, b + 1)

            @pl.when(b > 0)
            def _():
                for copy in put(0, i):
                    copy.wait()

            r = rows_of(i)
            hids = []
            for j in range(NJ):
                c = pl.ds(j * CL, CL)
                gate, up = (dot(a_s[r, :], columns_of(now_w, m, j)) for m in BOTH)
                held[i, 0, :, c] = gate
                held[i, 1, :, c] = up
                hids.append((gate * jax.nn.sigmoid(gate) * up).astype(bf16))
            for copy in put(b, i):
                copy.start()
            for j in range(NJ):
                acc[r, :] += dot(hids[j], rows_of_down(now_wd, j))

        loop(NC, chunk)

    loop(blocks, block1)
    plan.slot()
    plan.need([(s, "done") for s in gathers[T]])
    now()
    fetch_next(1, 0)
    put_at.wait()

    def join(r):
        h_s[r, :] += acc[r, :].astype(bf16)
        norm(r)

    over_rows(join)
    for i in range(NC):
        for copy in put(0, i):
            copy.wait()
    plan.slot(3.0)
    now()

    for b in range(blocks):
        if b and b % NB == 0:
            start_scatter()
        for i in range(NC + 1):
            plan.slot(SECOND_US if i < NC else GRADIENTS_US)
            if i == END and b % NB == NB - 1 and b < LAST:
                plan.need([(s, "done") for s in gathers[b // NB + 1 + T]])
            if i == NC and b and b % NB == 0:
                plan.need([(s, "begun") for s in scatters[-1]])
                if b == DEEP * NB:
                    plan.need([(s, "free") for s in scatters[0]])
    slots2 = plan.take()

    def block2(b):
        await_block(b)
        now_w, now_wd = w.at[odd(b)], wd.at[odd(b)]

        def chunk(i):
            run_slot(slots2, b * (NC + 1) + i)

            @pl.when(b < LAST)
            def _():
                @pl.when(i == END)
                def _():
                    fetch_next(1, b + 1)

            r = rows_of(i)
            a = a_s[r, :]
            dy = dh_s[r, :]
            da = acc[r, :]
            for j in range(NJ):
                c = pl.ds(j * CL, CL)
                gate, up = (dot(a, columns_of(now_w, m, j)) for m in BOTH)
                hid, dup, dgate = parts(gate, up, dot_nt(dy, rows_of_down(now_wd, j)))
                dgate_s[r, c] = dgate
                dup_s[r, c] = dup
                hid_t[c, r] = hid.T
            for j in range(NJ):
                c = pl.ds(j * CL, CL)
                da += dot_nt(dgate_s[r, c], columns_of(now_w, 0, j)) + dot_nt(dup_s[r, c], columns_of(now_w, 1, j))
            acc[r, :] = da

        loop(NC, chunk)
        run_slot(slots2, b * (NC + 1) + NC)
        gradients_step(co, (at_s, dh_s, dgate_s, dup_s, hid_t), (wide_s, down_s), scratch, lax.div(b, NB), lax.rem(b, NB), DEEP)

    loop(blocks, block2)

    def norm_back(r):
        h = h_s[r, :].astype(f32)
        da = acc[r, :].astype(bf16).astype(f32)
        scale = lax.rsqrt(jnp.mean(h**2, -1, keepdims=True) + EPS)
        inner = jnp.mean(da * h, -1, keepdims=True)
        dh_s[r, :] += (da * scale - h * (inner * scale * scale * scale)).astype(bf16)

    over_rows(norm_back)
    last = T - 1
    for m in MATS:
        other, sems = scratch[m][0].at[last % DEEP], scratch[m][SCRATCH - 2].at[last]
        await_bytes(other, sems.at[SWAP_RECV])
        await_bytes(other, sems.at[SWAP_SEND])
    outs = [(dh_s, dh_ref), (wide_s.at[last % DEEP], wide_kept), (down_s.at[last % DEEP], down_kept)] + [(scratch[m][0].at[last % DEEP], other_kept[m]) for m in MATS]
    outs = [pltpu.make_async_copy(src, dst, dsems.at[i]) for i, (src, dst) in enumerate(outs)]
    for copy in outs:
        copy.start()
    plan.slot()
    plan.need([(s, "end") for stage in gathers + scatters for s in stage])
    now()
    for copy in outs:
        copy.wait()
    await_bytes(others.at[:, 0], xsems.at[0])
    await_bytes(others.at[:, rest], xsems.at[2])


FIRST_US = 1.5
SECOND_US = 2.5
THIRD_US = 0.9
GRADIENTS_US = 2.7
DEVICES = 256
BEGIN = 3
DEEP = 2
SETTLE = 3.0
VMEM = 67043328


def backward_kernel(down1, gate_ref, up_ref, at_ref, wide_kept, down_kept, *refs):
    other_kept, refs = refs[:3], refs[3:]
    dh_ref, sums1, dsums1, rows_out, down_out, total_out, *refs = refs
    scratch = [refs[SCRATCH * m : SCRATCH * (m + 1)] for m in MATS]
    at_s, dgate_s, dup_s, hid_t, wd, held, wide_s, down_s, sums, dsums, going, *refs = refs[SCRATCH * 3 :]
    slots_a, slots_b, wsems, hsems, lsems, xsems, psems, dsems = refs
    co = Here()
    planes = [plane_peers(co, axes) for axes in PLANES]
    blocks = T * NB
    ins = [(at_ref, at_s), (wide_kept, wide_s.at[0]), (down_kept, down_s.at[0])] + [(other_kept[m], scratch[m][0].at[0]) for m in MATS]
    ins = [pltpu.make_async_copy(src, dst, lsems.at[i]) for i, (src, dst) in enumerate(ins)]

    def down(b):
        return fetch({2: down1.at[lax.div(b, NB)]}, lax.rem(b, NB), (), wd.at[odd(b)], wsems.at[odd(b)])

    def saved(b, i):
        return [pltpu.make_async_copy(ref.at[b, i], held.at[i, k], hsems.at[i, k]) for k, ref in enumerate((gate_ref, up_ref))]

    for copy in ins + down(0) + [copy for i in range(NC) for copy in saved(0, i)]:
        copy.start()
    greet(axis_peers(co) + [co.partner] + [device for _, device in co.group] + planes[0][1] + planes[1][1] + piece_peers(co.index))
    early = T - 1
    for n in range(early):
        dsums[n, 1] = dsums1[n]
        for m in BOTH:
            sums[n, m] = sums1[n, m]
    for copy in ins:
        copy.wait()
    plan, scatters = Plan([]), []

    def start_scatter(swapped, start):
        def out(n, m):
            n += early
            return sums.at[n, m] if m < 2 else dsums.at[n % T, 1 - n // T]

        scatter_stage(plan, scatters, co, (wide_s, down_s), scratch, out, swapped, T + 1, T + 1, T, start)

    start_scatter(False, 0.0)
    for b in range(blocks):
        if b and b % NB == 0:
            start_scatter(True, plan.now + SETTLE)
        for i in range(NC + 1):
            plan.slot(THIRD_US if i < NC else GRADIENTS_US)
            if i == NC and b and b % NB == 0:
                plan.need([(s, "begun") for s in scatters[-1]])
                if b == early * NB:
                    plan.need([(s, "free") for s in scatters[0]])
    slots3 = plan.take()
    start_scatter(True, plan.now + SETTLE)
    plan.slot()
    plan.need([(s, "end") for stage in scatters for s in stage])

    def block3(b):
        for copy in down(b):
            copy.wait()

        @pl.when(b < LAST)
        def _():
            for copy in down(b + 1):
                copy.start()

        def chunk(i):
            run_slot(slots3, b * (NC + 1) + i)
            for copy in saved(b, i):
                copy.wait()
            r = rows_of(i)
            dh = dh_ref[r, :]
            for j in range(NJ):
                c = pl.ds(j * CL, CL)
                hid, dup, dgate = parts(held[i, 0, :, c], held[i, 1, :, c], dot_nt(dh, rows_of_down(wd.at[odd(b)], j)))
                dgate_s[r, c] = dgate
                dup_s[r, c] = dup
                hid_t[c, r] = hid.T

            @pl.when(b < LAST)
            def _():
                for copy in saved(b + 1, i):
                    copy.start()

        loop(NC, chunk)
        run_slot(slots3, b * (NC + 1) + NC)
        gradients_step(co, (at_s, dh_ref, dgate_s, dup_s, hid_t), (wide_s, down_s), scratch, 1 + lax.div(b, NB), lax.rem(b, NB), T)

    loop(blocks, block3)
    for tick in plan.take()[0]:
        tick()
    finish(co, sums, dsums, going, rows_out, down_out, total_out, (slots_a, slots_b), planes, xsems, psems, dsems)


def finish(co, sums, dsums, going, rows_out, down_out, total_out, planes, groups, xsems, psems, dsems):
    mine, here = co.mine, co.index
    stages = sums.shape[0]
    start_pieces(dsums, down_out, here, dsems, False)

    def fill(n):
        for m in BOTH:
            for j in range(SIZE):
                going[j, n, pl.ds(PER * m, PER), :] = sums[n, m, pl.ds(PER * j, PER), :]

    loop(stages, fill)
    copies = [remote(going.at[j], rows_out.at[mine], xsems.at[0], xsems.at[1], device) for j, device in co.group]
    for copy in copies:
        copy.start()
    rows_out[pl.ds(mine, 1)] = going[pl.ds(mine, 1)]
    square = jnp.sum((sums[...] * sums[...]).reshape(-1, 8, CL), axis=0)
    piece = jnp.sum((dsums[...] * dsums[...]).reshape(-1, 8, D), axis=0)
    square = sum(s[:, i : i + LANES] for s in (square, piece) for i in range(0, s.shape[1], LANES))
    for n, (slots, (me, peers)) in enumerate(zip(planes, groups)):
        slots[me] = square
        for device in peers:
            remote(slots.at[me], slots.at[me], psems.at[2 * n], psems.at[2 * n + 1], device).start()
        others = slots.at[upto(len(peers))]
        await_bytes(others, psems.at[2 * n + 1])
        await_bytes(others, psems.at[2 * n])
        square = jnp.sum(slots[...], axis=0)
    total_out[...] = jnp.full(total_out.shape, jnp.sum(square), f32)
    rest = rows_out.at[upto(SIZE - 1)]
    for n in BOTH:
        await_bytes(rest, xsems.at[n])
    await_pieces(dsums, down_out, here, dsems, False)


def hbm():
    return pl.BlockSpec(memory_space=pltpu.HBM)


def vmem():
    return pl.BlockSpec(memory_space=pltpu.VMEM)


TALL, FLAT, BLOCK = (TOKENS, D), (D, TOKENS), (TOKENS, FB)


def forward(rows, down, x, dy):
    stages = 2 * T
    full = [jax.ShapeDtypeStruct((T,) + DIMS + shape, bf16) for shape in SHAPES]
    kept = jax.ShapeDtypeStruct((T * NB, NC, RC, FB), f32)
    partial = [jax.ShapeDtypeStruct(s, bf16) for s in ((2,) + XYZ + CHUNK, XYZ + PIECE)]
    small = [jax.ShapeDtypeStruct(s, f32) for s in ((DEEP, 2) + CHUNK, (DEEP,) + PIECE)]
    return pl.pallas_call(
        forward_kernel,
        out_shape=full * 2 + [kept] * 2 + [jax.ShapeDtypeStruct(s, bf16) for s in (FLAT, TALL)] + partial + [jax.ShapeDtypeStruct(XYZ + s, bf16) for s in SHAPES] + small,
        in_specs=[vmem(), vmem(), hbm(), hbm()],
        out_specs=[hbm()] * 15 + [vmem()] * 2,
        scratch_shapes=scatter_scratch(DEEP)
        + [
            pltpu.VMEM(rows.shape, f32),
            pltpu.VMEM(CHUNK, f32),
            pltpu.VMEM((stages, 2) + CHUNK, bf16),
            pltpu.VMEM((T, 2) + PIECE, bf16),
            pltpu.VMEM(TALL, bf16),
            pltpu.VMEM(FLAT, bf16),
            pltpu.VMEM(TALL, bf16),
            pltpu.VMEM(TALL, bf16),
            pltpu.VMEM(TALL, f32),
            pltpu.VMEM(BLOCK, bf16),
            pltpu.VMEM(BLOCK, bf16),
            pltpu.VMEM(BLOCK[::-1], bf16),
            pltpu.VMEM((2,) + WIDE, bf16),
            pltpu.VMEM((2,) + DIMS[1:] + PIECE, bf16),
            pltpu.VMEM((NC, 2, RC, FB), f32),
            pltpu.VMEM((DEEP + 1, 2) + XYZ + CHUNK, bf16),
            pltpu.VMEM((DEEP + 1,) + XYZ + PIECE, bf16),
        ]
        + [pltpu.SemaphoreType.DMA(s) for s in ((stages, 3, SEMS), (2, 3, 2), (NC, 2), (2,), (4,), (stages,))],
        compiler_params=pltpu.CompilerParams(collective_id=1, has_side_effects=True, vmem_limit_bytes=VMEM),
        name="forward",
    )(rows, down, x, dy)


def backward(down1, kept, at, partial, dh, sums, shape):
    planes = (16, 8, LANES)
    return pl.pallas_call(
        backward_kernel,
        out_shape=[jax.ShapeDtypeStruct(s, f32) for s in (shape, (T, 2) + PIECE, (8, LANES))],
        in_specs=[hbm()] * 9 + [vmem()] * 3,
        out_specs=[vmem()] * 3,
        scratch_shapes=scatter_scratch(T)
        + [
            pltpu.VMEM(FLAT, bf16),
            pltpu.VMEM(BLOCK, bf16),
            pltpu.VMEM(BLOCK, bf16),
            pltpu.VMEM(BLOCK[::-1], bf16),
            pltpu.VMEM((2,) + DIMS[1:] + PIECE, bf16),
            pltpu.VMEM((NC, 2, RC, FB), f32),
            pltpu.VMEM((T + 1, 2) + XYZ + CHUNK, bf16),
            pltpu.VMEM((T + 1,) + XYZ + PIECE, bf16),
        ]
        + [pltpu.VMEM(s, f32) for s in ((2 * T, 2) + CHUNK, (T, 2) + PIECE, shape, planes, planes)]
        + [pltpu.SemaphoreType.DMA(s) for s in ((2, 3, 2), (NC, 2), (2 * T,), (4,), (4,), (2 * T,))],
        compiler_params=pltpu.CompilerParams(collective_id=2, has_side_effects=True, vmem_limit_bytes=VMEM),
        name="backward",
    )(down1, *kept, at, *partial, dh, *sums)


def adamw(w, m, v, g):
    m = 0.9 * m + 0.1 * g
    v = 0.95 * v + 0.05 * g * g
    step = m * lax.rsqrt(v + 1e-8) + 0.1 * w
    return (w - 0.02 * step).astype(bf16), m, v


def solution(mesh):
    def step(x, dy, w_gate, w_up, w_down, *moments):
        m, v = moments[:3], moments[3:]
        weights = (w_gate, w_up, w_down)
        rows = jnp.stack([w_gate, w_up], 1).reshape(2, 2 * PER, T, SIZE, CL).transpose(3, 0, 2, 1, 4).reshape(SIZE, 2 * T, 2 * PER, CL)
        rows = jnp.pad(rows.astype(f32), ((0, 0), (0, 0), (0, 2), (0, 0)))
        down = w_down.reshape((2, T) + PIECE).transpose(1, 0, 2, 3)
        *full, gate, up, at, dh, wide, narrow, other0, other1, other2, sums, dsums = forward(rows, down, x[0], dy[0])
        rows, down, total = backward(full[2], (gate, up), at, (wide, narrow, other0, other1, other2), dh, (sums, dsums), rows.shape)
        rows = rows[:, :, : 2 * PER].reshape(SIZE, 2, T, 2, PER, CL).transpose(3, 1, 4, 2, 0, 5)[:, ::-1].reshape((2,) + w_gate.shape)
        down = down.transpose(1, 0, 2, 3).reshape(w_down.shape)
        gradients = (rows[0], rows[1], down)
        count = 256 * sum(w.size for w in weights)
        factor = jnp.minimum(1.0, 0.5 * lax.rsqrt(total[0, 0] / count + 1e-30))
        new = [adamw(w.astype(f32), m, v, g * factor) for w, m, v, g in zip(weights, m, v, gradients, strict=True)]
        return tuple(one[which] for which in range(3) for one in new)

    states, cut = P(("rep", "dp"), None, None), P(None, "dp", None)
    return jax.shard_map(
        step,
        mesh=mesh,
        in_specs=(states, states) + (cut,) * 9,
        out_specs=(P("rep", "dp", None),) * 9,
        check_vma=False,
    )
```

```python
import functools
import jax
import jax.numpy as jnp
from jax import lax
from jax.experimental import pallas as pl
from jax.experimental.pallas import tpu as pltpu
from jax.sharding import PartitionSpec as P

DIMS = (4, 4, 8, 2)
T = 3
CH, CL, DR, D = 24, 256, 8, 768
CHUNK, PIECE = (CH, CL), (DR, D)
SHAPES = (CHUNK, CHUNK, PIECE)
XYZ = DIMS[:3]
SIZE, PER = 8, 3
ORDERS = ((0, 1, 2), (2, 1, 0), (2, 0, 1))
MATS = range(len(ORDERS))
WAYS = (1, -1)
BOTH = range(2)
f32, bf16 = jnp.float32, jnp.bfloat16
ALL = slice(None)
LANES = CL // 2
LINK = CH * CL * 2 / 46.6e3
TICK = 0.2
HOP = 3.3


def apart(n):
    return range(1, n)


def part(half):
    return 0.5 if half else 1.0


def flat(co):
    r = co[0]
    for n, i in zip(DIMS[1:], co[1:]):
        r = r * n + i
    return r


class Here(list):
    def __init__(self):
        r = lax.axis_index("dp")
        self.index = r
        for n in DIMS[::-1]:
            self.insert(0, lax.rem(r, n))
            r = lax.div(r, n)
        self.pos, self.dev = [], []
        for axis, n in enumerate(DIMS):
            self.pos.append([self[axis]] + [lax.rem(self[axis] + k, n) for k in apart(n)])
            self.dev.append([flat(self[:axis] + [p] + self[axis + 1 :]) for p in self.pos[axis]])
        self.partner = self.dev[3][1]
        half = SIZE // 2
        z = lax.rem(self[2], half)
        base = self.index - z * 2 - self[3]
        self.mine = z * 2 + self[3]
        self.group = [(j, base + j) for j in (lax.rem(self.mine + k, SIZE) for k in apart(SIZE))]


def place(co, axis, by):
    return co.pos[axis][by % DIMS[axis]]


def peer(co, axis, by):
    return co.dev[axis][by % DIMS[axis]]


def axis_peers(co):
    return [co.dev[a][k] for a in MATS for k in apart(DIMS[a])]


def plane_peers(co, axes):
    (i, m), (j, n) = ((co[a], DIMS[a]) for a in axes)
    strides = [flat([int(a == b) for b in range(len(DIMS))]) for a in axes]
    me = i * n + j
    base = co.index - i * strides[0] - j * strides[1]
    others = [lax.rem(me + k, m * n) for k in apart(m * n)]
    return me, [base + lax.div(o, n) * strides[0] + lax.rem(o, n) * strides[1] for o in others]


PLANES = ((2, 3), (0, 1))


def greet(peers):
    barrier = pltpu.get_barrier_semaphore()
    for peer in peers:
        pl.semaphore_signal(barrier, inc=1, device_id={"dp": peer})
    pl.semaphore_wait(barrier, len(peers))


def remote(src, dst, ssem, rsem, device):
    return pltpu.make_async_remote_copy(src_ref=src, dst_ref=dst, send_sem=ssem, recv_sem=rsem, device_id={"dp": device})


def loop(n, body, lo=0):
    def step(i, _):
        body(i)
        return 0

    lax.fori_loop(lo, lo + n, step, 0)


def await_bytes(view, sem):
    pltpu.make_async_copy(view, view, sem).wait()


def upto(n):
    return pl.ds(0, n)


def side(by):
    return (1 - by) // 2


def cut(n, half):
    return ALL if half is ALL else pl.ds(half * (n // 2), n // 2)


(KEEP, SWAP_SEND, SWAP_RECV, RING_SEND, SEND1, RECV1, SEND2, RECV2), RING_RECV = range(8), 8
SEND3, RECV3 = SEND1, RECV1
SEMS = 16


def far(n):
    return n * n / 8


class Stream:
    def __init__(self, after=()):
        self.ticks, self.after, self.next, self.ready, self.marks = [], after, 0, 0.0, {}

    def add(self, run, axis=-1, load=0.0, travel=0.0, after=()):
        self.ticks.append((run, axis, load, travel, after))

    def mark(self, name):
        self.marks[name] = len(self.ticks)

    def passed(self, name):
        return self.next >= self.marks[name]


def at(ref, sel, core=ALL):
    index = list(sel) + ([] if core is ALL else [core])
    return ref.at[tuple(index)]


def gather_stream(ref, own, order, co, sems, after, ready):
    s = Stream(after)
    c = co[3]
    a1, a2, a3 = order
    n1, n2, n3 = (DIMS[a] for a in order)

    def sel(i, j, k):
        out = [0, 0, 0]
        out[a1], out[a2], out[a3] = i, j, k
        return out

    mine = at(ref, co[:3], c)
    keep = lambda: pltpu.make_async_copy(own, mine, sems.at[KEEP])
    block2 = lambda: at(ref, sel(ALL, co[a2], co[a3]), c)

    def block3(k, half=ALL):
        return at(ref, sel(cut(n1, half), ALL, k), c)

    def forward(view):
        remote(view, view, sems.at[SWAP_SEND], sems.at[SWAP_RECV], co.partner).start()

    def spread(source, target, n, axis, i, j):
        for k in apart(n):
            remote(source, target, sems.at[i], sems.at[j], peer(co, axis, k)).start()

    def one():
        ready()
        keep().start()
        spread(own, mine, n1, a1, SEND1, RECV1)

    def two():
        await_bytes(at(ref, sel(upto(n1 - 1), 0, 0), c), sems.at[RECV1])
        keep().wait()
        spread(block2(), block2(), n2, a2, SEND2, RECV2)

    def ring(step, by):
        half = side(by) if step == n3 // 2 else ALL
        view = block3(place(co, a3, -by * (step - 1)), half)
        came = block3(place(co, a3, -by * step), half)
        return remote(view, view, sems.at[RING_SEND], sems.at[RING_RECV + 2 * step - 1 - side(by)], peer(co, a3, by)), came

    def three(step):
        if step == 1:
            await_bytes(at(ref, sel(ALL, upto(n2 - 1), 0), c), sems.at[RECV2])
        for by in WAYS:
            if step > 1:
                ring(step - 1, by)[0].wait_recv()
            if step <= n3 // 2:
                ring(step, by)[0].start()
        if step == 1:
            forward(block3(co[a3]))
        else:
            for by in WAYS:
                forward(ring(step - 1, by)[1])

    def finish():
        half = at(ref, [ALL] * 3, 1 - c)
        await_bytes(half, sems.at[SWAP_RECV])

    def drain():
        half = at(ref, [ALL] * 3, c)
        await_bytes(half, sems.at[SWAP_SEND])
        await_bytes(at(ref, sel(upto(n1 - 1), 0, 0), c), sems.at[SEND1])
        await_bytes(at(ref, sel(ALL, upto(n2 - 1), 0), c), sems.at[SEND2])
        await_bytes(at(ref, sel(ALL, ALL, upto(n3 - 1)), c), sems.at[RING_SEND])

    s.add(one, a1, far(n1) * LINK, HOP + n1 / 8)
    s.add(two, a2, far(n2) * n1 * LINK, HOP + n2 / 8)
    for step in range(1, n3 // 2 + 1):
        s.add(functools.partial(three, step), a3, n1 * n2 * LINK * part(step == n3 // 2), HOP)
    s.add(functools.partial(three, n3 // 2 + 1), travel=2.0)
    s.add(finish)
    s.mark("done")
    s.add(drain)
    s.mark("end")
    return s


def swap_block(partial, other, m, b, co, sems):
    for half in range(2 if m < 2 else 1):
        index = (ALL, ALL, half * 4 + b) if m < 2 else (b,)
        remote(partial.at[index], other.at[index], sems.at[SWAP_SEND], sems.at[SWAP_RECV], co.partner).start()


def scatter_scratch(deep, stages):
    out = []
    for order, shape in zip(ORDERS, SHAPES):
        n2, n3 = DIMS[order[1]], DIMS[order[0]]
        out += [
            pltpu.VMEM((deep,) + XYZ + shape, bf16),
            pltpu.VMEM((deep,) + XYZ + shape, bf16),
            pltpu.VMEM((n3,) + shape, f32),
            pltpu.VMEM((n2, n3) + shape, bf16),
            pltpu.VMEM((2, n2 - 1, n3) + shape, bf16),
            pltpu.VMEM((2, n3 - 1) + shape, bf16),
            pltpu.SemaphoreType.DMA((stages, SEMS)),
            pltpu.SemaphoreType.REGULAR((len(WAYS) + 1,)),
        ]
    return out


SCRATCH = 8


def scatter_stream(kept, order, co, scratch, out, stage, swapped, swaps, rings, before):
    other, came1, total, going, came2, came3, sems, free = scratch
    deep = other.shape[0]
    other, came1 = other.at[stage % deep], came1.at[stage % deep]
    came2, came3, sems = came2.at[stage % 2], came3.at[stage % 2], sems.at[stage]
    s = Stream()
    b3, b2, b1 = order
    n1, n2, n3 = (DIMS[a] for a in (b1, b2, b3))
    p1, p2, p3 = (co[a] for a in (b1, b2, b3))
    mid = n1 // 2

    def sel(q, i=ALL, j=ALL):
        out = [0, 0, 0]
        out[b1], out[b2], out[b3] = q, i, j
        return out

    def chunk_sum(refs, q, i):
        return sum(r[tuple(sel(q, i))].astype(f32) for r in refs)

    def sums(q, lo, size, refs):
        def body(i):
            kept[tuple(sel(q, i))] = chunk_sum(refs, q, i).astype(bf16)

        loop(size, body, lo)

    def ring(step, by):
        q = place(co, b1, by * (mid + 1 - step))
        slot = place(co, b1, mid - 1) if by < 0 and step == mid else q
        half = side(by) if step == 1 else ALL
        view, target = at(kept, sel(q, cut(n2, half))), at(came1, sel(slot, cut(n2, half)))
        return remote(view, target, sems.at[RING_SEND], sems.at[RING_RECV + 2 * step - 1 - side(by)], peer(co, b1, by))

    def around(step):
        if step == 1 and swapped:
            await_bytes(other, sems.at[SWAP_RECV])
            await_bytes(other, sems.at[SWAP_SEND])
        for by in WAYS:
            q = place(co, b1, by * (mid + 1 - step))
            if step == 1:
                if stage >= deep:
                    pl.semaphore_wait(free.at[1 + side(by)], 1)
                sums(q, side(by) * (n2 // 2), n2 // 2, (kept, other))
            else:
                ring(step - 1, by).wait_recv()
                if step == 2:
                    sums(q, side(by) * (n2 // 2), n2 // 2, (kept, other, came1))
                    sums(q, side(-by) * (n2 // 2), n2 // 2, (kept, other))
                else:
                    sums(q, 0, n2, (kept, other, came1))
            ring(step, by).start()

    def middle():
        for by in WAYS:
            ring(mid, by).wait_recv()
        opposite = place(co, b1, mid)

        def value(i):
            return chunk_sum((kept, other, came1), p1, i) + came1[tuple(sel(opposite, i))].astype(f32)

        def body(i):
            going[i] = value(i).astype(bf16)

        loop(n2, body)
        total[...] = value(p2)
        for k in apart(n2):
            remote(going.at[place(co, b2, k)], came2.at[k - 1], sems.at[SEND2], sems.at[RECV2], peer(co, b2, k)).start()
        if stage + deep < rings:
            for by in WAYS:
                pl.semaphore_signal(free.at[1 + side(-by)], inc=1, device_id={"dp": peer(co, b1, by)})
        if stage + deep < swaps:
            pl.semaphore_signal(free.at[0], inc=1, device_id={"dp": co.partner})

    def release():
        await_bytes(at(came1, sel(upto(n1 - 1))), sems.at[RING_SEND])

    def late():
        await_bytes(came2, sems.at[RECV2])
        await_bytes(came2, sems.at[SEND2])
        value = total[...] + jnp.sum(came2[...].astype(f32), axis=0)
        total[...] = value
        going[p2] = value.astype(bf16)
        for k in apart(n3):
            remote(going.at[p2, place(co, b3, k)], came3.at[k - 1], sems.at[SEND3], sems.at[RECV3], peer(co, b3, k)).start()

    def last():
        await_bytes(came3, sems.at[RECV3])
        value = total[p3] + jnp.sum(came3[...].astype(f32), axis=0)
        out[...] = value.astype(bf16).astype(f32)
        await_bytes(came3, sems.at[SEND3])

    for step in range(1, mid + 1):
        s.add(functools.partial(around, step), b1, n2 * n3 * LINK * part(step == 1), HOP + 0.7)
        s.marks.setdefault("begun", len(s.ticks))
    s.add(middle, b2, far(n2) * n3 * LINK, HOP + n2 / 8, [(p, "end") for p in before])
    s.mark("middle")
    s.add(release)
    s.mark("free")
    s.add(late, b3, far(n3) * LINK, HOP + n3 / 8)
    s.add(last)
    s.mark("end")
    return s


class Plan:
    def __init__(self, streams):
        self.streams, self.busy, self.now, self.slots, self.done = streams, [0.0] * 4, 0.0, [], {}

    def open(self, s):
        return s.next < len(s.ticks) and all(other.passed(name) for other, name in (*s.after, *s.ticks[s.next][-1]))

    def run(self, s):
        run, axis, load, travel, _ = s.ticks[s.next]
        self.slots[-1].append(run)
        self.now += TICK
        begin = max(self.now, self.busy[axis])
        if load:
            self.busy[axis] = begin + load
        s.next += 1
        s.ready = begin + load + travel

    def slot(self, length=0.0):
        self.slots.append([])
        more = True
        while more:
            more = False
            for s in self.streams:
                if self.open(s) and s.ready <= self.now:
                    self.run(s)
                    more = True
        self.now += length

    def need(self, wanted):
        while not all(s.passed(name) for s, name in wanted):
            s = min((s for s in self.streams if self.open(s)), key=lambda s: s.ready)
            self.now = max(self.now, s.ready)
            self.run(s)

    def take(self):
        out, self.slots = self.slots, []
        return out


def only(slots, step, where):
    return [ticks if q % step in where else () for q, ticks in enumerate(slots)]


def run_slot(slots, index, fold=8):
    for lo in range(0, len(slots), fold):
        some = slots[lo : lo + fold]
        if any(some):

            def inner(lo=lo, some=some):
                for i, ticks in enumerate(some):
                    if ticks:

                        @pl.when(index == lo + i)
                        def _(ticks=ticks):
                            for tick in ticks:
                                tick()

            pl.when(lax.div(index, fold) == lo // fold)(inner)

TOKENS = 1024
FB = 512
NJ = FB // CL
NB = 4
RC = 512
NC = TOKENS // RC
END = NC - 1
EPS = 1e-6
NORM = 256
LAST = T * NB - 1
WIDE = (2, 4, 4, 2, 2) + CHUNK


def dot(a, b):
    return jnp.dot(a, b, preferred_element_type=f32)


def dot_nt(a, b):
    return lax.dot_general(a, b, (((1,), (1,)), ((), ())), preferred_element_type=f32)


def odd(b):
    return lax.rem(b, 2)


def rows_of(i, n=RC):
    return pl.ds(pl.multiple_of(i * n, n), n)


def over_rows(body):
    loop(TOKENS // NORM, lambda i: body(rows_of(i, NORM)))


def normed(h):
    wide = h.astype(f32)
    scale = lax.rsqrt(jnp.mean(wide**2, -1, keepdims=True) + EPS)
    return (wide * scale).astype(bf16)


def fetch(refs, b, w, wd, sems):
    out = []
    for m in MATS:
        if m in refs:
            ref = refs[m]
            if m < 2:
                for half in BOTH:
                    out.append(pltpu.make_async_copy(ref.at[:, :, half * 4 + b], w.at[m, :, :, half], sems.at[m, half]))
            else:
                out.append(pltpu.make_async_copy(ref.at[b], wd, sems.at[m, 0]))
    return out


def rows_of_down(wd, j):
    return wd[pl.ds(2 * j, 2)].reshape(CL, D)


def columns_of(w, m, j):
    return w[m, :, :, :, j].reshape(D, CL)


def pieces(device):
    return [(lax.rem(T * device + i, DEVICES), lax.div(T * device + i, DEVICES)) for i in range(T)]


def origins(device):
    return [(lax.div(DEVICES * t + device, T), lax.rem(DEVICES * t + device, T)) for t in range(T)]


def piece_peers(here):
    return [d for d, _ in pieces(here) + origins(here)]


def routes(out, here):
    return [(i, *to) for i, to in enumerate(pieces(here) if out else origins(here))]


def start_piece(src, dst, here, sems, route):
    i, device, slot = route

    @pl.when(device != here)
    def _():
        remote(src.at[i], dst.at[slot], sems.at[i], sems.at[T + slot], device).start()

    @pl.when(device == here)
    def _():
        dst[slot] = src[i]


def await_pieces(src, dst, here, sems, out):
    for i, device, _ in routes(out, here):

        @pl.when(device != here)
        def _(i=i):
            await_bytes(src.at[i], sems.at[i])

    for i, device, _ in routes(not out, here):

        @pl.when(device != here)
        def _(i=i):
            await_bytes(dst.at[i], sems.at[T + i])


def parts(gate, up, dhid):
    s = jax.nn.sigmoid(gate)
    silu = gate * s
    wide = dhid.astype(bf16).astype(f32)
    hid = (silu * up).astype(bf16)
    dup = (wide * silu).astype(bf16)
    dgate = (wide * up * (s + silu * (1.0 - s))).astype(bf16)
    return hid, dup, dgate


def weight_gradients(at_s, dh_s, dgate, dup, hid_t, wide, down, slots, b, between):
    half = D // 2
    for m, src in enumerate((dgate, dup)):
        for i in BOTH:
            for j in range(NJ):
                value = dot(at_s[pl.ds(i * half, half), :], src[:, pl.ds(j * CL, CL)]).reshape((2, 4, 2) + CHUNK).astype(bf16)
                for z in BOTH:
                    wide[slots[j], m, pl.ds(2 * i, 2), :, z * 4 + b] = value[:, :, z]
    between()
    for j in range(NJ):
        value = dot(hid_t[pl.ds(j * CL, CL), :], dh_s[...]).reshape((2, 8, 2) + PIECE).astype(bf16)
        for c in BOTH:
            down[slots[c], b, pl.ds(2 * j, 2)] = value[:, :, c]


def gradients_step(co, tensors, buffers, scratch, stage, b, deep, between):
    wide_s, down_s = buffers
    slot = lax.rem(stage, deep)
    slots = [slot * me + deep * (1 - me) for me in (1 - co[3], co[3])]
    weight_gradients(*tensors, wide_s, down_s, slots, b, between)

    @pl.when(stage >= deep)
    def _():
        @pl.when(b == 0)
        def _():
            for m in MATS:
                pl.semaphore_wait(scratch[m][SCRATCH - 1].at[0], 1)

    for m in MATS:
        swap_block(wide_s.at[deep, m] if m < 2 else down_s.at[deep], scratch[m][0].at[slot], m, b, co, scratch[m][SCRATCH - 2].at[stage])


def scatter_stage(plan, scatters, co, buffers, scratch, sums, swapped, swaps, rings, deep, start):
    n = len(scatters)
    stage = []
    for m in MATS:
        before = [scatters[n - 1][m]] if n else []
        kept = buffers[0].at[n % deep, m] if m < 2 else buffers[1].at[n % deep]
        stage.append(scatter_stream(kept, ORDERS[m], co, scratch[m], sums(n, m), n, swapped, swaps, rings, before))
        stage[m].ready = start
    scatters.append(stage)
    plan.streams += stage


def forward_kernel(rows_ref, down_ref, x_ref, dy_ref, *refs):
    full, refs = (refs[:3], refs[3:6]), refs[6:]
    gate_ref, up_ref, at_ref, dh_ref, wide_kept, down_kept, *refs = refs
    other_kept, refs = refs[:3], refs[3:]
    sums, dsums, *refs = refs
    scratch = [refs[SCRATCH * m : SCRATCH * (m + 1)] for m in MATS]
    got, wide, chunks, eights, a_s, at_s, h_s, dh_s, acc, dgate_s, dup_s, hid_t, w, wd, held, wide_s, down_s, *refs = refs[SCRATCH * 3 :]
    gsems, wsems, hsems, lsems, xsems, dsems = refs
    co = Here()
    mine, here = co.mine, co.index
    greet(axis_peers(co) + [co.partner] + [device for _, device in co.group] + piece_peers(here))

    stages = 2 * T
    rest = pl.ds(1, stages - 1)

    def swap(j, device, part, i):
        return remote(rows_ref.at[j, part], got.at[mine, part], xsems.at[i], xsems.at[i + 1], device)

    for part, i in ((0, 0), (rest, 2)):
        for j, device in co.group:
            swap(j, device, part, i).start()
        if i == 0:
            for route in routes(True, here):
                start_piece(down_ref, eights, here, dsems, route)
    loads = [pltpu.make_async_copy(src, dst, lsems.at[i]) for i, (src, dst) in enumerate(((x_ref, h_s), (dy_ref, dh_s)))]
    for copy in loads:
        copy.start()
    got[pl.ds(mine, 1)] = rows_ref[pl.ds(mine, 1)]
    others = got.at[upto(SIZE - 1)]

    def own(n):
        for m in BOTH:
            for j in range(SIZE):
                wide[pl.ds(PER * j, PER), :] = got[j, n, pl.ds(m * PER, PER), :]
            chunks[n, m] = wide[...].astype(bf16)

    await_bytes(others.at[:, 0], xsems.at[1])
    own(0)
    gathers, scatters = [], []
    for n in range(stages):
        after = [(s, "begin") for s in gathers[n - 1]] if n else []
        l, t = n // T, n % T
        stage = []
        for m in MATS:
            chunk = chunks.at[n, m] if m < 2 else eights.at[t, l]
            ready = (lambda: await_pieces(down_ref, eights, here, dsems, True)) if m == 2 and n == 0 else lambda: ()
            stage.append(gather_stream(full[l][m].at[t], chunk, ORDERS[m], co, gsems.at[n, m], after, ready))
        for s in stage:
            s.marks["begin"] = GATES[n]
        gathers.append(stage)
    soon, *later = gathers
    plan = Plan(list(soon))

    def now():
        for ticks in plan.take():
            for tick in ticks:
                tick()

    def start_scatter():
        scatter_stage(plan, scatters, co, (wide_s, down_s), scratch, lambda n, m: sums.at[n, m] if m < 2 else dsums.at[n], True, T, DEEP, DEEP, plan.now + SETTLE)

    plan.slot(6.0)
    now()
    for copy in loads:
        copy.wait()

    def norm(r):
        a = normed(h_s[r, :])
        a_s[r, :] = a
        at_s[:, r] = a.T
        acc[r, :] = jnp.zeros((NORM, D), f32)

    over_rows(norm)
    put_at = pltpu.make_async_copy(at_s, at_ref, lsems.at[0])
    put_at.start()
    await_bytes(others.at[:, rest], xsems.at[3])
    for n in apart(stages):
        own(n)
    plan.streams += [s for stage in later for s in stage]
    plan.slot()
    plan.need([(s, "done") for s in gathers[0]])
    now()

    def weights(layer, t, b):
        return fetch(dict(enumerate(ref.at[t] for ref in full[layer])), lax.rem(b, NB), w.at[odd(b)], wd.at[odd(b)], wsems.at[odd(b)])

    def fetch_next(layer, b):
        for copy in weights(layer, lax.div(b, NB), b):
            copy.start()

    def await_block(b):
        for copy in weights(0, 0, b):
            copy.wait()

    fetch_next(0, 0)
    blocks = T * NB
    for b in range(blocks):
        for i in range(NC):
            plan.slot(FIRST_US)
            if i == END and b % NB == NB - 1 and b < LAST:
                plan.need([(s, "done") for s in gathers[b // NB + 1]])
    slots1 = plan.take()

    def put(b, i):
        return [pltpu.make_async_copy(held.at[i, k], ref.at[b, i], hsems.at[i, k]) for k, ref in enumerate((gate_ref, up_ref))]

    def block1(b):
        await_block(b)
        now_w, now_wd = w.at[odd(b)], wd.at[odd(b)]

        def chunk(i):
            run_slot(slots1, b * NC + i)

            @pl.when(b < LAST)
            def _():
                @pl.when(i == lax.div(lax.rem(b, NB), NB - 1) * (END))
                def _():
                    fetch_next(0, b + 1)

            @pl.when(b > 0)
            def _():
                for copy in put(0, i):
                    copy.wait()

            r = rows_of(i)
            hids = []
            for j in range(NJ):
                c = pl.ds(j * CL, CL)
                gate, up = (dot(a_s[r, :], columns_of(now_w, m, j)) for m in BOTH)
                held[i, 0, :, c] = gate
                held[i, 1, :, c] = up
                hids.append((gate * jax.nn.sigmoid(gate) * up).astype(bf16))
            for copy in put(b, i):
                copy.start()
            for j in range(NJ):
                acc[r, :] += dot(hids[j], rows_of_down(now_wd, j))

        loop(NC, chunk)

    loop(blocks, block1)
    plan.slot()
    plan.need([(s, "done") for s in gathers[T]])
    now()
    fetch_next(1, 0)
    put_at.wait()

    def join(r):
        h_s[r, :] += acc[r, :].astype(bf16)
        norm(r)

    over_rows(join)
    for i in range(NC):
        for copy in put(0, i):
            copy.wait()
    plan.slot(3.0)
    now()

    for b in range(blocks):
        if b and b % NB == 0:
            start_scatter()
        for i in range(SLOTS):
            plan.slot(SECOND_US if i < NC else GRADIENTS_US)
            if i == END and b % NB == NB - 1 and b < LAST:
                plan.need([(s, "done") for s in gathers[b // NB + 1 + T]])
            if i == NC and b and b % NB == 0:
                plan.need([(s, "begun") for s in scatters[-1]])
                if b == DEEP * NB:
                    plan.need([(s, "free") for s in scatters[0]])
    slots2 = plan.take()

    def block2(b):
        await_block(b)
        now_w, now_wd = w.at[odd(b)], wd.at[odd(b)]

        def chunk(i):
            run_slot(only(slots2, SLOTS, range(NC)), b * SLOTS + i)

            @pl.when(b < LAST)
            def _():
                @pl.when(i == END)
                def _():
                    fetch_next(1, b + 1)

            r = rows_of(i)
            a = a_s[r, :]
            dy = dh_s[r, :]
            da = acc[r, :]
            for j in range(NJ):
                c = pl.ds(j * CL, CL)
                gate, up = (dot(a, columns_of(now_w, m, j)) for m in BOTH)
                hid, dup, dgate = parts(gate, up, dot_nt(dy, rows_of_down(now_wd, j)))
                dgate_s[r, c] = dgate
                dup_s[r, c] = dup
                hid_t[c, r] = hid.T
            for j in range(NJ):
                c = pl.ds(j * CL, CL)
                da += dot_nt(dgate_s[r, c], columns_of(now_w, 0, j)) + dot_nt(dup_s[r, c], columns_of(now_w, 1, j))
            acc[r, :] = da

        loop(NC, chunk)
        run_slot(only(slots2, SLOTS, [NC]), b * SLOTS + NC)
        gradients_step(co, (at_s, dh_s, dgate_s, dup_s, hid_t), (wide_s, down_s), scratch, lax.div(b, NB), lax.rem(b, NB), DEEP, lambda: run_slot(only(slots2, SLOTS, [NC + 1]), b * SLOTS + NC + 1))

    loop(blocks, block2)

    def norm_back(r):
        h = h_s[r, :].astype(f32)
        da = acc[r, :].astype(bf16).astype(f32)
        scale = lax.rsqrt(jnp.mean(h**2, -1, keepdims=True) + EPS)
        inner = jnp.mean(da * h, -1, keepdims=True)
        dh_s[r, :] += (da * scale - h * (inner * scale * scale * scale)).astype(bf16)

    over_rows(norm_back)
    last = DEEP
    for m in MATS:
        other, sems = scratch[m][0].at[last % DEEP], scratch[m][SCRATCH - 2].at[last]
        await_bytes(other, sems.at[SWAP_RECV])
        await_bytes(other, sems.at[SWAP_SEND])
    outs = [(dh_s, dh_ref), (wide_s.at[last % DEEP], wide_kept), (down_s.at[last % DEEP], down_kept)] + [(scratch[m][0].at[last % DEEP], other_kept[m]) for m in MATS]
    outs = [pltpu.make_async_copy(src, dst, dsems.at[i]) for i, (src, dst) in enumerate(outs)]
    for copy in outs:
        copy.start()
    plan.slot()
    plan.need([(s, "end") for stage in gathers + scatters for s in stage])
    now()
    for copy in outs:
        copy.wait()
    await_bytes(others.at[:, 0], xsems.at[0])
    await_bytes(others.at[:, rest], xsems.at[2])


FIRST_US = 1.5
SECOND_US = 2.5
THIRD_US = 0.9
GRADIENTS_US = 1.35
SLOTS = NC + 2
DEVICES = 256
GATES = (1, 2, 1, 4, 4, 2)
DEEP = 2
LATE = T + 1
SETTLE = 2.0
VMEM = 67043328


def backward_kernel(down1, gate_ref, up_ref, at_ref, wide_kept, down_kept, *refs):
    other_kept, refs = refs[:3], refs[3:]
    dh_ref, sums1, dsums1, rows_out, down_out, total_out, *refs = refs
    scratch = [refs[SCRATCH * m : SCRATCH * (m + 1)] for m in MATS]
    at_s, dgate_s, dup_s, hid_t, wd, held, wide_s, down_s, sums, dsums, going, *refs = refs[SCRATCH * 3 :]
    slots_a, slots_b, squares, wsems, hsems, lsems, xsems, psems, dsems = refs
    co = Here()
    planes = [plane_peers(co, axes) for axes in PLANES]
    blocks = T * NB
    ins = [(at_ref, at_s), (wide_kept, wide_s.at[0]), (down_kept, down_s.at[0])] + [(other_kept[m], scratch[m][0].at[0]) for m in MATS]
    ins = [pltpu.make_async_copy(src, dst, lsems.at[i]) for i, (src, dst) in enumerate(ins)]

    def down(b):
        return fetch({2: down1.at[lax.div(b, NB)]}, lax.rem(b, NB), (), wd.at[odd(b)], wsems.at[odd(b)])

    def saved(b, i):
        return [pltpu.make_async_copy(ref.at[b, i], held.at[i, k], hsems.at[i, k]) for k, ref in enumerate((gate_ref, up_ref))]

    for copy in ins + down(0) + [copy for i in range(NC) for copy in saved(0, i)]:
        copy.start()
    greet(axis_peers(co) + [co.partner] + [device for _, device in co.group] + planes[0][1] + planes[1][1] + piece_peers(co.index))
    early = DEEP
    way = routes(False, co.index)

    def give(n):
        piece = dsums[n % T, 1 - n // T]
        square = jnp.sum(sums[n] * sums[n], axis=0).reshape(T, 8, CL).sum(axis=0)
        squares[...] += sum(s[:, i : i + LANES] for s in (square, piece * piece) for i in range(0, s.shape[1], LANES))
        for m in BOTH:
            for j in range(SIZE):
                going[j, n, pl.ds(PER * m, PER), :] = sums[n, m, pl.ds(PER * j, PER), :]
        for j, device in co.group:
            remote(going.at[j, n], rows_out.at[co.mine, n], xsems.at[0], xsems.at[1], device).start()
        rows_out[co.mine, n] = going[co.mine, n]
        if n >= T:
            start_piece(dsums, down_out, co.index, dsems, way[n - T])

    squares[...] = jnp.zeros_like(squares)
    for n in range(early):
        dsums[n, 1] = dsums1[n]
        for m in BOTH:
            sums[n, m] = sums1[n, m]
        give(n)
    for copy in ins:
        copy.wait()
    plan, scatters, ends = Plan([]), [], []

    def start_scatter(swapped, start):
        def out(n, m):
            n += early
            return sums.at[n, m] if m < 2 else dsums.at[n % T, 1 - n // T]

        scatter_stage(plan, scatters, co, (wide_s, down_s), scratch, out, swapped, LATE, LATE, T, start)
        ends.append(Stream([(s, "end") for s in scatters[-1]]))
        ends[-1].add(functools.partial(give, early + len(ends) - 1))
        ends[-1].mark("end")
        plan.streams.append(ends[-1])

    start_scatter(False, 0.0)
    for b in range(blocks):
        if b and b % NB == 0:
            start_scatter(True, plan.now + SETTLE)
        for i in range(SLOTS):
            plan.slot(THIRD_US if i < NC else GRADIENTS_US)
            if i == NC and b and b % NB == 0:
                plan.need([(s, "begun") for s in scatters[-1]])
                if b == early * NB:
                    plan.need([(s, "free") for s in scatters[0]])
    slots3 = plan.take()
    start_scatter(True, plan.now + SETTLE)
    plan.slot()
    plan.need([(s, "end") for s in ends])

    def block3(b):
        for copy in down(b):
            copy.wait()

        @pl.when(b < LAST)
        def _():
            for copy in down(b + 1):
                copy.start()

        def chunk(i):
            run_slot(only(slots3, SLOTS, range(NC)), b * SLOTS + i)
            for copy in saved(b, i):
                copy.wait()
            r = rows_of(i)
            dh = dh_ref[r, :]
            for j in range(NJ):
                c = pl.ds(j * CL, CL)
                hid, dup, dgate = parts(held[i, 0, :, c], held[i, 1, :, c], dot_nt(dh, rows_of_down(wd.at[odd(b)], j)))
                dgate_s[r, c] = dgate
                dup_s[r, c] = dup
                hid_t[c, r] = hid.T

            @pl.when(b < LAST)
            def _():
                for copy in saved(b + 1, i):
                    copy.start()

        loop(NC, chunk)
        run_slot(only(slots3, SLOTS, [NC]), b * SLOTS + NC)
        gradients_step(co, (at_s, dh_ref, dgate_s, dup_s, hid_t), (wide_s, down_s), scratch, 1 + lax.div(b, NB), lax.rem(b, NB), T, lambda: run_slot(only(slots3, SLOTS, [NC + 1]), b * SLOTS + NC + 1))

    loop(blocks, block3)
    for tick in plan.take()[0]:
        tick()
    square = squares[...]
    for n, (slots, (me, peers)) in enumerate(zip((slots_a, slots_b), planes)):
        slots[me] = square
        for device in peers:
            remote(slots.at[me], slots.at[me], psems.at[2 * n], psems.at[2 * n + 1], device).start()
        others = slots.at[upto(len(peers))]
        await_bytes(others, psems.at[2 * n + 1])
        await_bytes(others, psems.at[2 * n])
        square = jnp.sum(slots[...], axis=0)
    total_out[...] = jnp.full(total_out.shape, jnp.sum(square), f32)
    rest = rows_out.at[upto(SIZE - 1)]
    for n in BOTH:
        await_bytes(rest, xsems.at[n])
    await_pieces(dsums, down_out, co.index, dsems, False)


def hbm():
    return pl.BlockSpec(memory_space=pltpu.HBM)


def vmem():
    return pl.BlockSpec(memory_space=pltpu.VMEM)


TALL, FLAT, BLOCK = (TOKENS, D), (D, TOKENS), (TOKENS, FB)


def forward(rows, down, x, dy):
    stages = 2 * T
    full = [jax.ShapeDtypeStruct((T,) + DIMS + shape, bf16) for shape in SHAPES]
    kept = jax.ShapeDtypeStruct((T * NB, NC, RC, FB), f32)
    partial = [jax.ShapeDtypeStruct(s, bf16) for s in ((2,) + XYZ + CHUNK, XYZ + PIECE)]
    small = [jax.ShapeDtypeStruct(s, f32) for s in ((DEEP, 2) + CHUNK, (DEEP,) + PIECE)]
    return pl.pallas_call(
        forward_kernel,
        out_shape=full * 2 + [kept] * 2 + [jax.ShapeDtypeStruct(s, bf16) for s in (FLAT, TALL)] + partial + [jax.ShapeDtypeStruct(XYZ + s, bf16) for s in SHAPES] + small,
        in_specs=[vmem(), vmem(), hbm(), hbm()],
        out_specs=[hbm()] * 15 + [vmem()] * 2,
        scratch_shapes=scatter_scratch(DEEP, T)
        + [
            pltpu.VMEM(rows.shape, f32),
            pltpu.VMEM(CHUNK, f32),
            pltpu.VMEM((stages, 2) + CHUNK, bf16),
            pltpu.VMEM((T, 2) + PIECE, bf16),
            pltpu.VMEM(TALL, bf16),
            pltpu.VMEM(FLAT, bf16),
            pltpu.VMEM(TALL, bf16),
            pltpu.VMEM(TALL, bf16),
            pltpu.VMEM(TALL, f32),
            pltpu.VMEM(BLOCK, bf16),
            pltpu.VMEM(BLOCK, bf16),
            pltpu.VMEM(BLOCK[::-1], bf16),
            pltpu.VMEM((2,) + WIDE, bf16),
            pltpu.VMEM((2,) + DIMS[1:] + PIECE, bf16),
            pltpu.VMEM((NC, 2, RC, FB), f32),
            pltpu.VMEM((T, 2) + XYZ + CHUNK, bf16),
            pltpu.VMEM((T,) + XYZ + PIECE, bf16),
        ]
        + [pltpu.SemaphoreType.DMA(s) for s in ((stages, 3, SEMS), (2, 3, 2), (NC, 2), (2,), (4,), (stages,))],
        compiler_params=pltpu.CompilerParams(collective_id=1, has_side_effects=True, vmem_limit_bytes=VMEM),
        name="forward",
    )(rows, down, x, dy)


def backward(down1, kept, at, partial, dh, sums, shape):
    planes = (16, 8, LANES)
    return pl.pallas_call(
        backward_kernel,
        out_shape=[jax.ShapeDtypeStruct(s, f32) for s in (shape, (T, 2) + PIECE, (8, LANES))],
        in_specs=[hbm()] * 9 + [vmem()] * 3,
        out_specs=[vmem()] * 3,
        scratch_shapes=scatter_scratch(T, LATE)
        + [
            pltpu.VMEM(FLAT, bf16),
            pltpu.VMEM(BLOCK, bf16),
            pltpu.VMEM(BLOCK, bf16),
            pltpu.VMEM(BLOCK[::-1], bf16),
            pltpu.VMEM((2,) + DIMS[1:] + PIECE, bf16),
            pltpu.VMEM((NC, 2, RC, FB), f32),
            pltpu.VMEM((LATE, 2) + XYZ + CHUNK, bf16),
            pltpu.VMEM((LATE,) + XYZ + PIECE, bf16),
        ]
        + [pltpu.VMEM(s, f32) for s in ((2 * T, 2) + CHUNK, (T, 2) + PIECE, shape, planes, planes, planes[1:])]
        + [pltpu.SemaphoreType.DMA(s) for s in ((2, 3, 2), (NC, 2), (2 * T,), (4,), (4,), (2 * T,))],
        compiler_params=pltpu.CompilerParams(collective_id=2, has_side_effects=True, vmem_limit_bytes=VMEM),
        name="backward",
    )(down1, *kept, at, *partial, dh, *sums)


def adamw(w, m, v, g):
    m = 0.9 * m + 0.1 * g
    v = 0.95 * v + 0.05 * g * g
    step = m * lax.rsqrt(v + 1e-8) + 0.1 * w
    return (w - 0.02 * step).astype(bf16), m, v


def solution(mesh):
    def step(x, dy, w_gate, w_up, w_down, *moments):
        m, v = moments[:3], moments[3:]
        weights = (w_gate, w_up, w_down)
        rows = jnp.stack([w_gate, w_up], 1).reshape(2, 2 * PER, T, SIZE, CL).transpose(3, 0, 2, 1, 4).reshape(SIZE, 2 * T, 2 * PER, CL)
        rows = jnp.pad(rows.astype(f32), ((0, 0), (0, 0), (0, 2), (0, 0)))
        down = w_down.reshape((2, T) + PIECE).transpose(1, 0, 2, 3)
        *full, gate, up, at, dh, wide, narrow, other0, other1, other2, sums, dsums = forward(rows, down, x[0], dy[0])
        rows, down, total = backward(full[2], (gate, up), at, (wide, narrow, other0, other1, other2), dh, (sums, dsums), rows.shape)
        rows = rows[:, :, : 2 * PER].reshape(SIZE, 2, T, 2, PER, CL).transpose(3, 1, 4, 2, 0, 5)[:, ::-1].reshape((2,) + w_gate.shape)
        down = down.transpose(1, 0, 2, 3).reshape(w_down.shape)
        gradients = (rows[0], rows[1], down)
        count = 256 * sum(w.size for w in weights)
        factor = jnp.minimum(1.0, 0.5 * lax.rsqrt(total[0, 0] / count + 1e-30))
        new = [adamw(w.astype(f32), m, v, g * factor) for w, m, v, g in zip(weights, m, v, gradients, strict=True)]
        return tuple(one[which] for which in range(3) for one in new)

    states, cut = P(("rep", "dp"), None, None), P(None, "dp", None)
    return jax.shard_map(
        step,
        mesh=mesh,
        in_specs=(states, states) + (cut,) * 9,
        out_specs=(P("rep", "dp", None),) * 9,
        check_vma=False,
    )
```
